128 devices in a mesh: row: 4 (over x_hi, core), col: 32 (over z, y, x_lo).
Axes of the slice: x: 4 (x_hi: 2, x_lo: 2; x = x_hi * 2 + x_lo), y: 4, z: 4, core: 2. Of those that a mesh axis runs over, the one named last changes fastest.
Arguments:
- rows: bfloat16 [4096, 4096], P(('row', 'col')), may hold values from -6 to 6
- task_ids: int32 [4096], P(('row', 'col')), may hold values from 0 to 8, as said below
- task_embed: bfloat16 [8, 4096], replicated, may hold values from -6 to 6
- norm_gain: float32 [4, 4096], replicated, may hold values from 0.1 to 1.9
- layer_weight: bfloat16 [4, 4096, 4096], P(None, None, 'col'), may hold values from -0.09375 to 0.09375
Outputs:
- packed_out: bfloat16 [4096, 4096], P('row', 'col')
The draws below stay inside these ranges and needn't reach their ends.
Inputs may be any that keep to these rules, and one draw needn't show every extreme that they name: `task_ids`: 8 marks an empty row, smaller values name a task.
All inputs are finite; a program needn't handle non-finite values.
Results may differ from the reference program's by a relative error of at most 0.008.
Values may be sent and summed in bfloat16 or wider, within the bound.
A program may use at most 128 MiB of HBM per device.

```python
import jax
import jax.numpy as jnp
from jax import lax

D = 4096
N_TASK = 8
LAYERS = 4
ROWS_DEV = 32
ROWS_TOTAL = 4096
N_ROW = 4
N_COL = 32


def draw_task_ids(key, part):
    first_key, second_key = jax.random.split(jax.random.fold_in(key, 11))
    device_count = N_ROW * N_COL
    live_rows = jax.random.randint(first_key, (device_count, 1), 3 * ROWS_DEV // 4, ROWS_DEV + 1)
    picked = jax.random.randint(second_key, (device_count, ROWS_DEV), 0, N_TASK)
    positions = jnp.arange(ROWS_DEV, dtype=jnp.int32)[None, :]
    table = jnp.where(positions < live_rows, picked, N_TASK)
    return table.reshape(-1).astype(jnp.int32)


def block_levels(rng, extent, cuts, least, largest):
    loudness = 1.0
    for position, blocks in cuts:
        draws = jax.random.uniform(jax.random.fold_in(jax.random.fold_in(rng, 6), position), (blocks,), jnp.float32, least / len(cuts), largest / len(cuts))
        loudness = loudness * jnp.repeat(jnp.exp(draws), extent[position] // blocks).reshape((-1,) + (1,) * (len(extent) - 1 - position))
    return loudness


def gaussian(key, extent, width, limit, shards=(), kind=jnp.bfloat16):
    drawn = jax.random.normal(key, extent, jnp.float32) * width
    if len(shards) > 0:
        drawn = block_levels(key, extent, shards, -0.22, 0.18) * drawn
    return jnp.clip(drawn, min=-limit, max=limit).astype(kind)


def setup_inputs(seed: int = 0) -> dict:
    streams_of = jax.random.split(jax.random.key(seed), 6)
    rows = gaussian(streams_of[0], (ROWS_TOTAL, D), 1.0, 6.0, ((0, 128),))
    task_ids = draw_task_ids(jax.random.fold_in(streams_of[5], 71), 0)
    task_embed = gaussian(streams_of[2], (N_TASK, D), 1.0, 6.0)
    norm_gain = jnp.clip(1.0 + 0.18 * jax.random.normal(streams_of[3], (LAYERS, D), jnp.float32), 0.1, 1.9)
    layer_weight = gaussian(streams_of[4], (LAYERS, D, D), D ** -0.5, 0.09375, ((2, 32),))
    return {"rows": rows, "task_ids": task_ids, "task_embed": task_embed, "norm_gain": norm_gain, "layer_weight": layer_weight}


epsilon = 1e-06

def reference(rows, task_ids, task_embed, norm_gain, layer_weight):
    device_count = N_ROW * N_COL
    row_total = device_count * ROWS_DEV
    task_table = task_ids.reshape(device_count, ROWS_DEV)
    task_range = jnp.arange(N_TASK, dtype=jnp.int32)
    member = (task_table[:, :, None] == task_range[None, None, :]).astype(jnp.int32)
    counts = lax.optimization_barrier(jnp.sum(member, axis=1)).astype(jnp.int32)
    before = (jnp.cumsum(counts, axis=0) - counts).astype(jnp.int32)
    totals = lax.optimization_barrier(jnp.sum(counts, axis=0)).astype(jnp.int32)
    task_base = (jnp.cumsum(totals) - totals).astype(jnp.int32)
    task_rank = lax.optimization_barrier(jnp.sum(member * (jnp.cumsum(member, axis=1) - member), axis=2)).astype(jnp.int32)
    packed_pos = (lax.optimization_barrier(jnp.sum(member * (task_base[None, None, :] + before[:, None, :]), axis=2)) + task_rank).astype(jnp.int32)
    target = jnp.where(task_table < N_TASK, packed_pos, row_total).reshape(-1).astype(jnp.int32)
    packed = jnp.zeros((row_total, D), jnp.bfloat16).at[target].set(rows, mode='drop')
    slot_pos = jnp.arange(row_total, dtype=jnp.int32)
    in_task = (slot_pos[:, None] >= task_base[None, :]) & (slot_pos[:, None] < (task_base + totals)[None, :])
    task_term = jnp.dot(in_task.astype(jnp.bfloat16), task_embed, preferred_element_type=jnp.float32)
    hidden = (packed.astype(jnp.float32) + task_term).astype(jnp.bfloat16)
    hidden = hidden.reshape(ROWS_DEV * N_COL, N_ROW, D).transpose(1, 0, 2).reshape(row_total, D)
    for layer_index in range(LAYERS):
        values = hidden.astype(jnp.float32)
        inverse_rms = lax.rsqrt(lax.optimization_barrier(jnp.mean(values * values, axis=1, keepdims=True)) + epsilon)
        active = jax.nn.silu(values * inverse_rms * norm_gain[layer_index][None, :]).astype(jnp.bfloat16)
        update = jnp.dot(active, layer_weight[layer_index], preferred_element_type=jnp.float32)
        hidden = (values + update).astype(jnp.bfloat16)
    return hidden
```

```python
import functools

import jax
import jax.numpy as jnp
from jax import lax
from jax.experimental import pallas as pl
from jax.experimental.pallas import tpu as pltpu
from jax.sharding import PartitionSpec as P

MESH = pl.DeviceIdType.MESH
F32 = jnp.float32
BF16 = jnp.bfloat16
EPS = 1e-06
LAYERS = 4
CUBE = [(1, 0, 0), (0, 1, 0), (0, 0, 1), (1, 1, 0), (0, 1, 1), (1, 0, 1), (1, 1, 1)]
NEXT = (1, 2, 0)
PREV = (2, 0, 1)
THIRDS = ((0, 3), (3, 3), (6, 2))
FAR = [(i // 4, (i // 2) % 2, i % 2) for i in range(1, 8)]


def flip(bit, on):
    return 1 - bit if on else bit


def kernel(
    rows_ref, ids_ref, embed_ref, gain_ref, w_ref, out_ref,
    wv, a, act, acc, h0s, h0, gp, pm, f, idg, idf, pos, stat, invb, oacc,
    wl, ws1s, ws1r, ws2s, ws2r, wds, wdr, a1s, a1r, a2s, a2r, a3s, a3r,
    hs, hr, i1s, i1r, i2s, i2r, i3s, i3r, sts, str_, fs, fr, fds, fdr,
):
    row, col = lax.axis_index("row"), lax.axis_index("col")
    xh, core = row // 2, row % 2
    z, y, x = col // 8, (col // 2) % 4, col % 2
    zh, zo, yh, yo = z // 2, z % 2, y // 2, y % 2
    zl, yl = zo + zh - 2 * zo * zh, yo + yh - 2 * yo * yh
    qme = zl * 4 + yl * 2 + x

    def cube_dev(fl):
        return (row, (zh * 2 + flip(zo, fl[2])) * 8 + (yh * 2 + flip(yo, fl[1])) * 2 + flip(x, fl[0]))

    def cube_q(fl):
        return flip(zl, fl[2]) * 4 + flip(yl, fl[1]) * 2 + flip(x, fl[0])

    def far_dev(fl):
        zz = 3 - z if fl[1] else z
        yy = 3 - y if fl[2] else y
        return (flip(xh, fl[0]) * 2 + core, zz * 8 + yy * 2 + x)

    def slot(fa, fb):
        return flip(zh, fa) * 2 + flip(yh, fb)

    def cols(s):
        return pl.ds(pl.multiple_of(s * 128, 128), 128)

    partner = (xh * 2 + (1 - core), col)
    links = [cube_dev(CUBE[d]) for d in range(3)]
    wlinks = [far_dev((0, 0, 1)), far_dev((0, 1, 0))]

    def remote(src, dst, ss, rs, dev):
        return pltpu.make_async_remote_copy(
            src_ref=src, dst_ref=dst, send_sem=ss, recv_sem=rs, device_id=dev, device_id_type=MESH
        )

    def both(ref, ss, rs, dev):
        return remote(ref, ref, ss, rs, dev)

    def load_own(l):
        for zz in range(4):
            for yy in range(4):
                q0 = min(zz, 3 - zz) * 4 + min(yy, 3 - yy) * 2
                pltpu.make_async_copy(
                    w_ref.at[l, zz, yy],
                    wv.at[l, pl.ds(q0, 2), (zz // 2) * 2 + yy // 2, :, cols(slot(0, 0))],
                    wl.at[l],
                ).start()

    def own_loaded(l):
        whole = wv.at[l, :, :, :, cols(slot(0, 0))]
        pltpu.make_async_copy(whole, whole, wl.at[l]).wait()

    def wpart(l, fa, fb, q0, n):
        return wv.at[l, pl.ds(q0, n), :, :, cols(slot(fa, fb))]

    def w1(l, k, j, recv=False):
        fa, fb = ((0, 1) if k == 0 else (1, 0)) if recv else (0, 0)
        return both(wpart(l, fa, fb, core * 4 + 2 * j, 2), ws1s.at[l, k, j], ws1r.at[l, k, j], wlinks[k])

    def w2(l, k, recv=False):
        fa, fb = (1, 1) if recv else ((1, 0) if k == 0 else (0, 1))
        return both(wpart(l, fa, fb, core * 4 + 2 * (1 - k), 2), ws2s.at[l, k], ws2r.at[l, k], wlinks[k])

    def wd(l, k, recv=False):
        fa, fb = ((0, 1), (1, 0), (1, 1))[k]
        half = (1 - core) if recv else core
        return both(wpart(l, fa, fb, half * 4, 4), wds.at[l, k], wdr.at[l, k], partner)

    def w1_send(l):
        own_loaded(l)
        for k, j in ((0, 0), (1, 1), (0, 1), (1, 0)):
            w1(l, k, j).start()

    def w1_first(l):
        w1(l, 0, 0, True).wait_recv()
        w1(l, 1, 1, True).wait_recv()
        w2(l, 1).start()
        w2(l, 0).start()

    def w1_rest(l):
        w1(l, 0, 1, True).wait_recv()
        wd(l, 0).start()
        w1(l, 1, 0, True).wait_recv()
        wd(l, 1).start()

    def w2_in(l):
        w2(l, 0, True).wait_recv()
        w2(l, 1, True).wait_recv()
        wd(l, 2).start()

    def wd_in(l):
        for k in range(3):
            wd(l, k, True).wait_recv()

    def zero(l):
        return isinstance(l, int)

    def chunk(l, fl, i):
        if zero(l):
            at = pl.ds(pl.multiple_of(flip(yo, fl[1]) * 64 + flip(x, fl[0]) * 32, 32), 32)
            return a.at[0, pl.ds(4 * i, 4), flip(zo, fl[2]), at, :]
        return a.at[l, cube_q(fl), i]

    def third(l, fl, e):
        if zero(l):
            at = pl.ds(pl.multiple_of(flip(yo, fl[1]) * 64 + flip(x, fl[0]) * 32, 32), 32)
            return a.at[0, pl.ds(*THIRDS[e]), flip(zo, fl[2]), at, :]
        if e == 2:
            return a.at[l, cube_q(fl), :, pl.ds(80, 48), :]
        return a.at[l, cube_q(fl), e, pl.ds(0, 80), :]

    ME, ALL = (0, 0, 0), (1, 1, 1)

    def pair(d):
        e = PREV[d]
        return tuple(int(k in (d, e)) for k in range(3))

    def s1(l, d, i, recv=False):
        return both(chunk(l, CUBE[d] if recv else ME, i), a1s.at[l, d, i], a1r.at[l, d, i], links[d])

    def s2(l, d, i, recv=False):
        return both(chunk(l, pair(d) if recv else CUBE[PREV[d]], i), a2s.at[l, d, i], a2r.at[l, d, i], links[d])

    def s3(l, d, recv=False):
        return both(third(l, ALL if recv else pair(PREV[d]), d), a3s.at[l, d], a3r.at[l, d], links[d])

    def step1(l):
        for i in range(2):
            for d in range(3):
                s1(l, d, i).start()

    def step2(l, i):
        for d in range(3):
            s1(l, d, i, True).wait_recv()
        for d in range(3):
            s2(l, d, i).start()

    def step3(l):
        for i in range(2):
            for d in range(3):
                s2(l, d, i, True).wait_recv()
        for d in range(3):
            s3(l, d).start()

    def step3_in(l):
        for d in range(3):
            s3(l, d, True).wait_recv()

    def stat_copy(l, k, recv=False):
        q = cube_q(CUBE[k]) if recv else qme
        return both(stat.at[l, q], sts.at[l, k], str_.at[l, k], cube_dev(CUBE[k]))

    def eye():
        return lax.broadcasted_iota(jnp.int32, (256, 256), 0) == lax.broadcasted_iota(jnp.int32, (256, 256), 1)

    def multiply(l, src, held):
        acc[...] = held.reshape(256, 512).astype(F32)

        def body(q, carry):
            acc[...] += jnp.dot(src(q), wv[l, q].reshape(512, 512), preferred_element_type=F32)
            return carry

        lax.fori_loop(0, 8, body, 0)
        new = acc[...].astype(BF16)
        a[l + 1, qme] = new.reshape(2, 128, 512)
        val = new.astype(F32)
        sq = val * val
        sq = (sq[:, 0:128] + sq[:, 128:256]) + (sq[:, 256:384] + sq[:, 384:512])
        total = jnp.sum(sq, axis=1, keepdims=True)
        line = jnp.sum(jnp.where(eye(), total, 0.0), axis=0, keepdims=True)
        stat[l + 1, qme] = jnp.broadcast_to(line, (8, 256))

    def read_stats(l):
        total = stat[l, 0]
        for q in range(1, 8):
            total = total + stat[l, q]
        half = 0.5 * lax.rsqrt(total[0:1] * (1.0 / 4096.0) + EPS)
        tall = jnp.sum(jnp.where(eye(), half, 0.0), axis=1, keepdims=True)
        invb[...] = jnp.broadcast_to(tall, (256, 128))

    def activate(l, q):
        for t in range(4):
            c = slice(t * 128, t * 128 + 128)
            u = a[l, q, :, :, c].reshape(256, 128).astype(F32) * invb[...] * gp[l, q, 0:1, c]
            act[q, :, c] = (u + u * jnp.tanh(u)).astype(BF16)

    def h_copy(k, recv=False):
        fl = CUBE[k] if recv else ME
        dst = h0.at[flip(zo, fl[2]), pl.ds(pl.multiple_of(flip(yo, fl[1]) * 64 + flip(x, fl[0]) * 32, 32), 32), :]
        src = dst if recv else h0s.at[cube_q(CUBE[k])]
        return remote(src, dst, hs.at[k], hr.at[k], cube_dev(CUBE[k]))

    def id1(k, recv=False):
        fl = CUBE[k] if recv else ME
        return both(
            idg.at[flip(zo, fl[2]), flip(yo, fl[1]) * 2 + flip(x, fl[0])], i1s.at[k], i1r.at[k], cube_dev(CUBE[k])
        )

    def far_at(fl):
        return (flip(xh, fl[0]) * 2 + core) * 2 + flip(zh, fl[1]), flip(yh, fl[2])

    def id2(k, recv=False):
        g, b = far_at(FAR[k] if recv else ME)
        dst = idf.at[g, :, b]
        return remote(dst if recv else idg, dst, i2s.at[k], i2r.at[k], far_dev(FAR[k]))

    def id3(k, recv=False):
        c = (1 - core) if recv else core
        return both(idf.at[pl.ds((k * 2 + c) * 2, 2)], i3s.at[k], i3r.at[k], partner)

    def out1(k, recv=False):
        g, b = far_at(FAR[k] if recv else ME)
        dst = f.at[g, :, b]
        src = dst if recv else a.at[LAYERS, qme, :, :, cols(slot(FAR[k][1], FAR[k][2]))]
        return remote(src, dst, fs.at[k], fr.at[k], far_dev(FAR[k]))

    def out2(k, recv=False):
        fl = ([ME] + FAR)[k]
        c = (1 - core) if recv else core
        g = (flip(xh, fl[0]) * 2 + c) * 2 + flip(zh, fl[1])
        return both(f.at[g, :, flip(yh, fl[2])], fds.at[k], fdr.at[k], partner)

    def positions():
        spread = idf[...].reshape(1024, 128).astype(F32).astype(BF16)
        k = lax.broadcasted_iota(jnp.int32, (32, 1024), 0)
        j = lax.broadcasted_iota(jnp.int32, (32, 1024), 1)
        pick = jnp.where((j // 32 == k) & (j % 8 == 0), 1.0, 0.0).astype(BF16)
        code = jnp.dot(pick, spread, preferred_element_type=F32)
        member = jnp.concatenate([jnp.where(code == 8.0 - t, 1.0, 0.0) for t in range(8)], axis=0).astype(BF16)
        i0 = lax.broadcasted_iota(jnp.int32, (128, 128), 0)
        i1 = lax.broadcasted_iota(jnp.int32, (128, 128), 1)
        upper = jnp.where(i0 < i1, 1.0, 0.0).astype(BF16)
        within = jnp.dot(member, upper, preferred_element_type=F32)
        count = jnp.dot(member, jnp.ones((128, 128), BF16), preferred_element_type=F32).astype(BF16)
        j0 = lax.broadcasted_iota(jnp.int32, (256, 256), 0)
        j1 = lax.broadcasted_iota(jnp.int32, (256, 256), 1)
        lower = jnp.where(j1 < j0, 1.0, 0.0).astype(BF16)
        place = jnp.dot(lower, count, preferred_element_type=F32) + within
        where = jnp.full((32, 128), -1.0, F32)
        for t in range(8):
            where = jnp.where(code == 8.0 - t, place[t * 32 : t * 32 + 32], where)
        for k in range(32):
            pos[k, 0:1, :] = where[k : k + 1]

    def selection(k0, k1):
        slots = (lax.broadcasted_iota(jnp.int32, (1024, 128), 0) * 4 + row).astype(F32)

        def body(k, carry):
            for half in range(2):
                hit = slots == pos[k * 2 + half, 0:1, :]
                pm[k, :, half * 128 : half * 128 + 128] = jnp.where(hit, 1.0, 0.0).astype(BF16)
            return carry

        lax.fori_loop(k0, k1, body, 0)

    for l in range(LAYERS):
        load_own(l)

    barrier = pltpu.get_barrier_semaphore()
    peers = [cube_dev(fl) for fl in CUBE] + [far_dev(fl) for fl in FAR] + [partner]
    for dev in peers:
        pl.semaphore_signal(barrier, inc=1, device_id=dev, device_id_type=MESH)
    pl.semaphore_wait(barrier, len(peers))

    w1_send(0)

    ids = 8.0 - ids_ref[...].astype(F32)
    i0 = lax.broadcasted_iota(jnp.int32, (32, 32), 0)
    i1 = lax.broadcasted_iota(jnp.int32, (32, 32), 1)
    code = jnp.sum(jnp.where(i0 == i1, ids, 0.0), axis=1, keepdims=True)
    own_rows = pl.ds(pl.multiple_of(yo * 64 + x * 32, 32), 32)
    square = jnp.zeros((32, 128), F32)
    tiles = [
        (q, s, ((q // 4 if s < 2 else 3 - q // 4) * 8 + ((q // 2) % 2 if s % 2 == 0 else 3 - (q // 2) % 2) * 2 + q % 2) * 128)
        for q in range(8)
        for s in range(4)
    ]
    for q, s, c in tiles:
        table = embed_ref[:, c : c + 128].astype(F32)
        term = jnp.zeros((32, 128), F32)
        for t in range(8):
            term = jnp.where(code == 8.0 - t, table[t : t + 1], term)
        start = (rows_ref[:, c : c + 128].astype(F32) + term).astype(BF16)
        h0s[q, :, s * 128 : s * 128 + 128] = start
        start = start.astype(F32)
        square = square + start * start
        for l in range(LAYERS):
            gp[l, q, 0:1, s * 128 : s * 128 + 128] = gain_ref[l : l + 1, c : c + 128]
    half = 0.5 * lax.rsqrt(jnp.sum(square, axis=1, keepdims=True) * (1.0 / 4096.0) + EPS)
    for q, s, c in tiles:
        lanes = slice(s * 128, s * 128 + 128)
        u = h0s[q, :, lanes].astype(F32) * half * gp[0, q, 0:1, lanes]
        a[0, q, zo, own_rows, lanes] = (u + u * jnp.tanh(u)).astype(BF16)
    step1(0)
    h0[zo, own_rows, :] = h0s[qme]
    for k in range(7):
        h_copy(k).start()
    lane = lax.broadcasted_iota(jnp.int32, (32, 128), 1)
    sub = lax.broadcasted_iota(jnp.int32, (32, 128), 0)
    line = jnp.sum(jnp.where(lane == sub + (col % 4) * 32, code, 0.0), axis=0, keepdims=True)
    idg[zo, yo * 2 + x] = jnp.broadcast_to(line, (8, 128)).astype(jnp.int32)
    for k in range(7):
        id1(k).start()

    step2(0, 0)
    w1_first(0)
    w1_send(1)
    step2(0, 1)
    for k in range(7):
        id1(k, True).wait_recv()
    g, b = far_at(ME)
    idf[g, :, b] = idg[...]
    for k in range(7):
        id2(k).start()
    for k in range(7):
        h_copy(k, True).wait_recv()
    step3(0)
    w1_rest(0)
    step3_in(0)
    w2_in(0)
    wd_in(0)
    multiply(0, lambda q: a[0, q].reshape(256, 512), h0[...])

    def layer(l, carry):
        for k in range(7):
            stat_copy(l, k).start()
        step1(l)
        w1_first(l)

        @pl.when(l < LAYERS - 1)
        def _():
            w1_send(l + 1)

        for k in range(7):
            stat_copy(l, k, True).wait_recv()
        read_stats(l)
        step2(l, 0)
        activate(l, qme)
        step2(l, 1)
        for d in range(3):
            activate(l, cube_q(CUBE[d]))
        w1_rest(l)
        step3(l)

        @pl.when(l == 1)
        def _():
            for k in range(7):
                id2(k, True).wait_recv()
            for k in range(2):
                id3(k).start()

        @pl.when(l == 2)
        def _():
            for k in range(2):
                id3(k, True).wait_recv()
            positions()

        @pl.when(l >= 2)
        def _():
            selection((l - 2) * 8, (l - 1) * 8)

        for d in range(3):
            activate(l, cube_q(pair(d)))
        w2_in(l)
        step3_in(l)
        activate(l, cube_q(ALL))
        wd_in(l)
        multiply(l, lambda q: act[q], a[l, qme])
        return carry

    lax.fori_loop(1, LAYERS, layer, 0)

    for k in range(7):
        out1(k).start()
    f[g, :, b] = a[LAYERS, qme, :, :, cols(slot(0, 0))]
    out2(0).start()
    for k in range(7):
        out1(k, True).wait_recv()
        out2(k + 1).start()
    for k in range(8):
        out2(k, True).wait_recv()
    oacc[...] = jnp.zeros_like(oacc)

    def place(k, carry):
        oacc[...] += jnp.dot(pm[k], f[k // 2, k % 2].reshape(256, 128), preferred_element_type=F32)
        return carry

    lax.fori_loop(0, 16, place, 0)
    out_ref[...] = oacc[...].astype(BF16)

    def drain(l, carry):
        for k in range(2):
            for j in range(2):
                w1(l, k, j).wait_send()
            w2(l, k).wait_send()
        for k in range(3):
            wd(l, k).wait_send()
        return carry

    lax.fori_loop(0, LAYERS, drain, 0)

    def drain_act(l):
        for d in range(3):
            for i in range(2):
                s1(l, d, i).wait_send()
                s2(l, d, i).wait_send()
            s3(l, d).wait_send()

    drain_act(0)

    def drain_layer(l, carry):
        drain_act(l)
        for k in range(7):
            stat_copy(l, k).wait_send()
        return carry

    lax.fori_loop(1, LAYERS, drain_layer, 0)
    for k in range(7):
        h_copy(k).wait_send()
        id1(k).wait_send()
        id2(k).wait_send()
        out1(k).wait_send()
    for k in range(2):
        id3(k).wait_send()
    for k in range(8):
        out2(k).wait_send()


def shards(rows, task_ids, task_embed, norm_gain, layer_weight):
    dma = pltpu.SemaphoreType.DMA
    vmem = pltpu.VMEM
    pairs = lambda *shape: [dma(shape), dma(shape)]
    return pl.pallas_call(
        kernel,
        out_shape=jax.ShapeDtypeStruct((1024, 128), BF16),
        in_specs=[pl.BlockSpec(memory_space=pltpu.VMEM)] * 4 + [pl.BlockSpec(memory_space=pl.ANY)],
        out_specs=pl.BlockSpec(memory_space=pltpu.VMEM),
        scratch_shapes=[
            vmem((4, 8, 4, 128, 512), BF16),
            vmem((5, 8, 2, 128, 512), BF16),
            vmem((8, 256, 512), BF16),
            vmem((256, 512), F32),
            vmem((8, 32, 512), BF16),
            vmem((2, 128, 512), BF16),
            vmem((4, 8, 8, 512), F32),
            vmem((16, 1024, 256), BF16),
            vmem((8, 2, 2, 128, 128), BF16),
            vmem((2, 4, 8, 128), jnp.int32),
            vmem((8, 2, 2, 4, 8, 128), jnp.int32),
            vmem((32, 8, 128), F32),
            vmem((5, 8, 8, 256), F32),
            vmem((256, 128), F32),
            vmem((1024, 128), F32),
            dma((4,)),
            *pairs(4, 2, 2),
            *pairs(4, 2),
            *pairs(4, 3),
            *pairs(4, 3, 2),
            *pairs(4, 3, 2),
            *pairs(4, 3),
            *pairs(7),
            *pairs(7),
            *pairs(7),
            *pairs(2),
            *pairs(4, 7),
            *pairs(7),
            *pairs(8),
        ],
        compiler_params=pltpu.CompilerParams(
            collective_id=0, has_side_effects=True, vmem_limit_bytes=60 * 1024 * 1024
        ),
    )(
        rows,
        task_ids.reshape(1, 32),
        task_embed,
        norm_gain,
        layer_weight.reshape(4, 4, 4, 2, 128, 128),
    )


def solution(mesh):
    return jax.shard_map(
        shards,
        mesh=mesh,
        in_specs=(P(("row", "col"), None), P(("row", "col")), P(), P(), P(None, None, "col")),
        out_specs=P("row", "col"),
        check_vma=False,
    )
```

```python
import functools

import jax
import jax.numpy as jnp
from jax import lax
from jax.experimental import pallas as pl
from jax.experimental.pallas import tpu as pltpu
from jax.sharding import PartitionSpec as P

MESH = pl.DeviceIdType.MESH
F32 = jnp.float32
BF16 = jnp.bfloat16
EPS = 1e-06
LAYERS = 4
CUBE = [(1, 0, 0), (0, 1, 0), (0, 0, 1), (1, 1, 0), (0, 1, 1), (1, 0, 1), (1, 1, 1)]
NEXT = (1, 2, 0)
PREV = (2, 0, 1)
THIRDS = ((0, 3), (3, 3), (6, 2))
FAR = [(i // 4, (i // 2) % 2, i % 2) for i in range(1, 8)]


def flip(bit, on):
    return 1 - bit if on else bit


def kernel(
    rows_in, ids_in, embed_in, gain_in, w_ref, out_ref,
    rows_ref, ids_ref, embed_ref, gain_ref, outv,
    wv, a, act, acc, h0s, h0, gp, pm, f, idg, idf, pos, stat, invb, oacc,
    inp, outs, wl, ws1s, ws1r, ws2s, ws2r, wds, wdr, a1s, a1r, a2s, a2r, a3s, a3r,
    hs, hr, i1s, i1r, i2s, i2r, i3s, i3r, sts, str_, fs, fr, fds, fdr,
):
    row, col = lax.axis_index("row"), lax.axis_index("col")
    xh, core = row // 2, row % 2
    z, y, x = col // 8, (col // 2) % 4, col % 2
    zh, zo, yh, yo = z // 2, z % 2, y // 2, y % 2
    zl, yl = zo + zh - 2 * zo * zh, yo + yh - 2 * yo * yh
    qme = zl * 4 + yl * 2 + x

    def cube_dev(fl):
        return (row, (zh * 2 + flip(zo, fl[2])) * 8 + (yh * 2 + flip(yo, fl[1])) * 2 + flip(x, fl[0]))

    def cube_q(fl):
        return flip(zl, fl[2]) * 4 + flip(yl, fl[1]) * 2 + flip(x, fl[0])

    def far_dev(fl):
        zz = 3 - z if fl[1] else z
        yy = 3 - y if fl[2] else y
        return (flip(xh, fl[0]) * 2 + core, zz * 8 + yy * 2 + x)

    def slot(fa, fb):
        return flip(zh, fa) * 2 + flip(yh, fb)

    def cols(s):
        return pl.ds(pl.multiple_of(s * 128, 128), 128)

    partner = (xh * 2 + (1 - core), col)
    links = [cube_dev(CUBE[d]) for d in range(3)]
    wlinks = [far_dev((0, 0, 1)), far_dev((0, 1, 0))]

    def remote(src, dst, ss, rs, dev):
        return pltpu.make_async_remote_copy(
            src_ref=src, dst_ref=dst, send_sem=ss, recv_sem=rs, device_id=dev, device_id_type=MESH
        )

    def both(ref, ss, rs, dev):
        return remote(ref, ref, ss, rs, dev)

    def load_own(l):
        for zz in range(4):
            for yy in range(4):
                q0 = min(zz, 3 - zz) * 4 + min(yy, 3 - yy) * 2
                pltpu.make_async_copy(
                    w_ref.at[l, zz, yy],
                    wv.at[l, pl.ds(q0, 2), (zz // 2) * 2 + yy // 2, :, cols(slot(0, 0))],
                    wl.at[l],
                ).start()

    def own_loaded(l):
        whole = wv.at[l, :, :, :, cols(slot(0, 0))]
        pltpu.make_async_copy(whole, whole, wl.at[l]).wait()

    def wpart(l, fa, fb, q0, n):
        return wv.at[l, pl.ds(q0, n), :, :, cols(slot(fa, fb))]

    def w1(l, k, j, recv=False):
        fa, fb = ((0, 1) if k == 0 else (1, 0)) if recv else (0, 0)
        return both(wpart(l, fa, fb, core * 4 + 2 * j, 2), ws1s.at[l, k, j], ws1r.at[l, k, j], wlinks[k])

    def w2(l, k, recv=False):
        fa, fb = (1, 1) if recv else ((1, 0) if k == 0 else (0, 1))
        return both(wpart(l, fa, fb, core * 4 + 2 * (1 - k), 2), ws2s.at[l, k], ws2r.at[l, k], wlinks[k])

    def wd(l, k, recv=False):
        fa, fb = ((0, 1), (1, 0), (1, 1))[k]
        half = (1 - core) if recv else core
        return both(wpart(l, fa, fb, half * 4, 4), wds.at[l, k], wdr.at[l, k], partner)

    def w1_send(l):
        own_loaded(l)
        for k, j in ((0, 0), (1, 1), (0, 1), (1, 0)):
            w1(l, k, j).start()

    def w1_first(l):
        w1(l, 0, 0, True).wait_recv()
        w1(l, 1, 1, True).wait_recv()
        w2(l, 1).start()
        w2(l, 0).start()

    def w1_rest(l):
        w1(l, 0, 1, True).wait_recv()
        wd(l, 0).start()
        w1(l, 1, 0, True).wait_recv()
        wd(l, 1).start()

    def w2_in(l):
        w2(l, 0, True).wait_recv()
        w2(l, 1, True).wait_recv()
        wd(l, 2).start()

    def wd_in(l):
        for k in range(3):
            wd(l, k, True).wait_recv()

    def zero(l):
        return isinstance(l, int)

    def chunk(l, fl, i):
        if zero(l):
            at = pl.ds(pl.multiple_of(flip(yo, fl[1]) * 64 + flip(x, fl[0]) * 32, 32), 32)
            return a.at[0, pl.ds(4 * i, 4), flip(zo, fl[2]), at, :]
        return a.at[l, cube_q(fl), i]

    def third(l, fl, e):
        if zero(l):
            at = pl.ds(pl.multiple_of(flip(yo, fl[1]) * 64 + flip(x, fl[0]) * 32, 32), 32)
            return a.at[0, pl.ds(*THIRDS[e]), flip(zo, fl[2]), at, :]
        if e == 2:
            return a.at[l, cube_q(fl), :, pl.ds(80, 48), :]
        return a.at[l, cube_q(fl), e, pl.ds(0, 80), :]

    ME, ALL = (0, 0, 0), (1, 1, 1)

    def pair(d):
        e = PREV[d]
        return tuple(int(k in (d, e)) for k in range(3))

    def s1(l, d, i, recv=False):
        return both(chunk(l, CUBE[d] if recv else ME, i), a1s.at[l, d, i], a1r.at[l, d, i], links[d])

    def s2(l, d, i, recv=False):
        return both(chunk(l, pair(d) if recv else CUBE[PREV[d]], i), a2s.at[l, d, i], a2r.at[l, d, i], links[d])

    def s3(l, d, recv=False):
        return both(third(l, ALL if recv else pair(PREV[d]), d), a3s.at[l, d], a3r.at[l, d], links[d])

    def step1(l):
        for i in range(2):
            for d in range(3):
                s1(l, d, i).start()

    def step2(l, i):
        for d in range(3):
            s1(l, d, i, True).wait_recv()
        for d in range(3):
            s2(l, d, i).start()

    def step3(l):
        for i in range(2):
            for d in range(3):
                s2(l, d, i, True).wait_recv()
        for d in range(3):
            s3(l, d).start()

    def step3_in(l):
        for d in range(3):
            s3(l, d, True).wait_recv()

    def stat_copy(l, k, recv=False):
        q = cube_q(CUBE[k]) if recv else qme
        return both(stat.at[l, q], sts.at[l, k], str_.at[l, k], cube_dev(CUBE[k]))

    def eye():
        return lax.broadcasted_iota(jnp.int32, (256, 256), 0) == lax.broadcasted_iota(jnp.int32, (256, 256), 1)

    def multiply(l, qs, src, first):
        total = jnp.dot(src(qs[0]), wv[l, qs[0]].reshape(512, 512), preferred_element_type=F32)
        for q in qs[1:]:
            total = total + jnp.dot(src(q), wv[l, q].reshape(512, 512), preferred_element_type=F32)
        acc[...] = total if first else acc[...] + total

    def finish(l, held):
        new = (held.reshape(256, 512).astype(F32) + acc[...]).astype(BF16)
        a[l + 1, qme] = new.reshape(2, 128, 512)
        val = new.astype(F32)
        sq = val * val
        sq = (sq[:, 0:128] + sq[:, 128:256]) + (sq[:, 256:384] + sq[:, 384:512])
        total = jnp.sum(sq, axis=1, keepdims=True)
        line = jnp.sum(jnp.where(eye(), total, 0.0), axis=0, keepdims=True)
        stat[l + 1, qme] = jnp.broadcast_to(line, (8, 256))

    def read_stats(l):
        total = stat[l, 0]
        for q in range(1, 8):
            total = total + stat[l, q]
        half = 0.5 * lax.rsqrt(total[0:1] * (1.0 / 4096.0) + EPS)
        tall = jnp.sum(jnp.where(eye(), half, 0.0), axis=1, keepdims=True)
        invb[...] = jnp.broadcast_to(tall, (256, 128))

    def activate(l, q):
        for t in range(4):
            c = slice(t * 128, t * 128 + 128)
            u = a[l, q, :, :, c].reshape(256, 128).astype(F32) * invb[...] * gp[l, q, 0:1, c]
            act[q, :, c] = (u + u * jnp.tanh(u)).astype(BF16)

    def h_copy(k, recv=False):
        fl = CUBE[k] if recv else ME
        dst = h0.at[flip(zo, fl[2]), pl.ds(pl.multiple_of(flip(yo, fl[1]) * 64 + flip(x, fl[0]) * 32, 32), 32), :]
        src = dst if recv else h0s.at[cube_q(CUBE[k])]
        return remote(src, dst, hs.at[k], hr.at[k], cube_dev(CUBE[k]))

    def id1(k, recv=False):
        fl = CUBE[k] if recv else ME
        return both(
            idg.at[flip(zo, fl[2]), flip(yo, fl[1]) * 2 + flip(x, fl[0])], i1s.at[k], i1r.at[k], cube_dev(CUBE[k])
        )

    def far_at(fl):
        return (flip(xh, fl[0]) * 2 + core) * 2 + flip(zh, fl[1]), flip(yh, fl[2])

    def id2(k, recv=False):
        g, b = far_at(FAR[k] if recv else ME)
        dst = idf.at[g, :, b]
        return remote(dst if recv else idg, dst, i2s.at[k], i2r.at[k], far_dev(FAR[k]))

    def id3(k, recv=False):
        c = (1 - core) if recv else core
        return both(idf.at[pl.ds((k * 2 + c) * 2, 2)], i3s.at[k], i3r.at[k], partner)

    def out1(k, recv=False):
        g, b = far_at(FAR[k] if recv else ME)
        dst = f.at[g, :, b]
        src = dst if recv else a.at[LAYERS, qme, :, :, cols(slot(FAR[k][1], FAR[k][2]))]
        return remote(src, dst, fs.at[k], fr.at[k], far_dev(FAR[k]))

    def out2(k, recv=False):
        fl = ([ME] + FAR)[k]
        c = (1 - core) if recv else core
        g = (flip(xh, fl[0]) * 2 + c) * 2 + flip(zh, fl[1])
        return both(f.at[g, :, flip(yh, fl[2])], fds.at[k], fdr.at[k], partner)

    def positions():
        spread = idf[...].reshape(1024, 128).astype(F32).astype(BF16)
        k = lax.broadcasted_iota(jnp.int32, (32, 1024), 0)
        j = lax.broadcasted_iota(jnp.int32, (32, 1024), 1)
        pick = jnp.where((j // 32 == k) & (j % 8 == 0), 1.0, 0.0).astype(BF16)
        code = jnp.dot(pick, spread, preferred_element_type=F32)
        member = jnp.concatenate([jnp.where(code == 8.0 - t, 1.0, 0.0) for t in range(8)], axis=0).astype(BF16)
        i0 = lax.broadcasted_iota(jnp.int32, (128, 128), 0)
        i1 = lax.broadcasted_iota(jnp.int32, (128, 128), 1)
        upper = jnp.where(i0 < i1, 1.0, 0.0).astype(BF16)
        within = jnp.dot(member, upper, preferred_element_type=F32)
        count = jnp.dot(member, jnp.ones((128, 128), BF16), preferred_element_type=F32).astype(BF16)
        j0 = lax.broadcasted_iota(jnp.int32, (256, 256), 0)
        j1 = lax.broadcasted_iota(jnp.int32, (256, 256), 1)
        lower = jnp.where(j1 < j0, 1.0, 0.0).astype(BF16)
        place = jnp.dot(lower, count, preferred_element_type=F32) + within
        where = jnp.full((32, 128), -1.0, F32)
        for t in range(8):
            where = jnp.where(code == 8.0 - t, place[t * 32 : t * 32 + 32], where)
        for k in range(32):
            pos[k, 0:1, :] = where[k : k + 1]

    def selection(k0, k1):
        slots = (lax.broadcasted_iota(jnp.int32, (1024, 128), 0) * 4 + row).astype(F32)

        def body(k, carry):
            for half in range(2):
                hit = slots == pos[k * 2 + half, 0:1, :]
                pm[k, :, half * 128 : half * 128 + 128] = jnp.where(hit, 1.0, 0.0).astype(BF16)
            return carry

        lax.fori_loop(k0, k1, body, 0)

    barrier = pltpu.get_barrier_semaphore()
    peers = [cube_dev(fl) for fl in CUBE] + [far_dev(fl) for fl in FAR] + [partner]
    for dev in peers:
        pl.semaphore_signal(barrier, inc=1, device_id=dev, device_id_type=MESH)
    inputs = [
        pltpu.make_async_copy(src, dst, inp.at[k])
        for k, (src, dst) in enumerate(
            ((ids_in, ids_ref), (rows_in, rows_ref), (embed_in, embed_ref), (gain_in, gain_ref))
        )
    ]
    for copy in inputs:
        copy.start()
    for l in range(LAYERS):
        load_own(l)

    inputs[0].wait()
    ids = 8.0 - ids_ref[...].astype(F32)
    i0 = lax.broadcasted_iota(jnp.int32, (32, 32), 0)
    i1 = lax.broadcasted_iota(jnp.int32, (32, 32), 1)
    code = jnp.sum(jnp.where(i0 == i1, ids, 0.0), axis=1, keepdims=True)
    lane = lax.broadcasted_iota(jnp.int32, (32, 128), 1)
    sub = lax.broadcasted_iota(jnp.int32, (32, 128), 0)
    line = jnp.sum(jnp.where(lane == sub + (col % 4) * 32, code, 0.0), axis=0, keepdims=True)
    idg[zo, yo * 2 + x] = jnp.broadcast_to(line, (8, 128)).astype(jnp.int32)
    for copy in inputs[1:]:
        copy.wait()
    own_rows = pl.ds(pl.multiple_of(yo * 64 + x * 32, 32), 32)
    square = jnp.zeros((32, 128), F32)
    tiles = [
        (q, s, ((q // 4 if s < 2 else 3 - q // 4) * 8 + ((q // 2) % 2 if s % 2 == 0 else 3 - (q // 2) % 2) * 2 + q % 2) * 128)
        for q in range(8)
        for s in range(4)
    ]
    for q, s, c in tiles:
        table = embed_ref[:, c : c + 128].astype(F32)
        term = jnp.zeros((32, 128), F32)
        for t in range(8):
            term = jnp.where(code == 8.0 - t, table[t : t + 1], term)
        start = (rows_ref[:, c : c + 128].astype(F32) + term).astype(BF16)
        h0s[q, :, s * 128 : s * 128 + 128] = start
        start = start.astype(F32)
        square = square + start * start
        for l in range(LAYERS):
            gp[l, q, 0:1, s * 128 : s * 128 + 128] = gain_ref[l : l + 1, c : c + 128]
    half = 0.5 * lax.rsqrt(jnp.sum(square, axis=1, keepdims=True) * (1.0 / 4096.0) + EPS)
    for q, s, c in tiles:
        lanes = slice(s * 128, s * 128 + 128)
        u = h0s[q, :, lanes].astype(F32) * half * gp[0, q, 0:1, lanes]
        a[0, q, zo, own_rows, lanes] = (u + u * jnp.tanh(u)).astype(BF16)
    h0[zo, own_rows, :] = h0s[qme]

    pl.semaphore_wait(barrier, len(peers))
    step1(0)
    w1_send(0)
    for k in range(7):
        id1(k).start()

    step2(0, 0)
    w1_first(0)
    w1_send(1)
    step2(0, 1)
    for k in range(7):
        h_copy(k).start()
    step3(0)
    for k in range(7):
        id1(k, True).wait_recv()
    g, b = far_at(ME)
    idf[g, :, b] = idg[...]
    for k in range(7):
        id2(k).start()
    w1_rest(0)
    step3_in(0)
    w2_in(0)
    wd_in(0)
    multiply(0, range(8), lambda q: a[0, q].reshape(256, 512), True)
    for k in range(7):
        h_copy(k, True).wait_recv()
    finish(0, h0[...])

    def layer(l, carry):
        for k in range(7):
            stat_copy(l, k).start()
        step1(l)
        w1_first(l)

        @pl.when(l < LAYERS - 1)
        def _():
            w1_send(l + 1)

        for k in range(7):
            stat_copy(l, k, True).wait_recv()
        read_stats(l)
        step2(l, 0)
        activate(l, qme)
        step2(l, 1)
        near = [cube_q(CUBE[d]) for d in range(3)]
        for q in near:
            activate(l, q)
        w1_rest(l)
        step3(l)

        @pl.when(l == 1)
        def _():
            for k in range(7):
                id2(k, True).wait_recv()
            for k in range(2):
                id3(k).start()

        @pl.when(l == 2)
        def _():
            for k in range(2):
                id3(k, True).wait_recv()
            positions()

        @pl.when(l >= 2)
        def _():
            selection((l - 2) * 8, (l - 1) * 8)

        mid = [cube_q(pair(d)) for d in range(3)]
        for q in mid:
            activate(l, q)
        w2_in(l)
        wd_in(l)
        multiply(l, [qme] + near + mid, lambda q: act[q], True)
        step3_in(l)
        activate(l, cube_q(ALL))
        multiply(l, [cube_q(ALL)], lambda q: act[q], False)
        finish(l, a[l, qme])
        return carry

    lax.fori_loop(1, LAYERS, layer, 0)

    for k in range(7):
        out1(k).start()
    f[g, :, b] = a[LAYERS, qme, :, :, cols(slot(0, 0))]
    out2(0).start()

    def place(first, last, groups):
        for m in range(4):
            lines = slice(m * 256, m * 256 + 256)
            total = None if first else oacc[lines]
            for at in groups:
                for k in range(2):
                    part = jnp.dot(
                        pm[at * 2 + k, lines], f[at, k].reshape(256, 128), preferred_element_type=F32
                    )
                    total = part if total is None else total + part
            if last:
                outv[lines] = total.astype(BF16)
                pltpu.make_async_copy(outv.at[lines], out_ref.at[lines], outs.at[m]).start()
            else:
                oacc[lines] = total

    for k in range(3):
        out1(k, True).wait_recv()
        out2(k + 1).start()
    place(True, False, [(xh * 2 + core) * 2 + k for k in range(2)])
    for k in range(3, 7):
        out1(k, True).wait_recv()
        out2(k + 1).start()
    place(False, False, [((1 - xh) * 2 + core) * 2 + k for k in range(2)])
    for k in range(8):
        out2(k, True).wait_recv()
    place(False, True, [(k // 2 * 2 + 1 - core) * 2 + k % 2 for k in range(4)])
    for m in range(4):
        lines = slice(m * 256, m * 256 + 256)
        pltpu.make_async_copy(outv.at[lines], out_ref.at[lines], outs.at[m]).wait()

    def drain(l, carry):
        for k in range(2):
            for j in range(2):
                w1(l, k, j).wait_send()
            w2(l, k).wait_send()
        for k in range(3):
            wd(l, k).wait_send()
        return carry

    lax.fori_loop(0, LAYERS, drain, 0)

    def drain_act(l):
        for d in range(3):
            for i in range(2):
                s1(l, d, i).wait_send()
                s2(l, d, i).wait_send()
            s3(l, d).wait_send()

    drain_act(0)

    def drain_layer(l, carry):
        drain_act(l)
        for k in range(7):
            stat_copy(l, k).wait_send()
        return carry

    lax.fori_loop(1, LAYERS, drain_layer, 0)
    for k in range(7):
        h_copy(k).wait_send()
        id1(k).wait_send()
        id2(k).wait_send()
        out1(k).wait_send()
    for k in range(2):
        id3(k).wait_send()
    for k in range(8):
        out2(k).wait_send()


def shards(rows, task_ids, task_embed, norm_gain, layer_weight):
    dma = pltpu.SemaphoreType.DMA
    vmem = pltpu.VMEM
    pairs = lambda *shape: [dma(shape), dma(shape)]
    return pl.pallas_call(
        kernel,
        out_shape=jax.ShapeDtypeStruct((1024, 128), BF16),
        in_specs=[pl.BlockSpec(memory_space=pl.ANY)] * 5,
        out_specs=pl.BlockSpec(memory_space=pl.ANY),
        scratch_shapes=[
            vmem((32, 4096), BF16),
            vmem((1, 32), jnp.int32),
            vmem((8, 4096), BF16),
            vmem((4, 4096), F32),
            vmem((1024, 128), BF16),
            vmem((4, 8, 4, 128, 512), BF16),
            vmem((5, 8, 2, 128, 512), BF16),
            vmem((8, 256, 512), BF16),
            vmem((256, 512), F32),
            vmem((8, 32, 512), BF16),
            vmem((2, 128, 512), BF16),
            vmem((4, 8, 8, 512), F32),
            vmem((16, 1024, 256), BF16),
            vmem((8, 2, 2, 128, 128), BF16),
            vmem((2, 4, 8, 128), jnp.int32),
            vmem((8, 2, 2, 4, 8, 128), jnp.int32),
            vmem((32, 8, 128), F32),
            vmem((5, 8, 8, 256), F32),
            vmem((256, 128), F32),
            vmem((1024, 128), F32),
            dma((4,)),
            dma((4,)),
            dma((4,)),
            *pairs(4, 2, 2),
            *pairs(4, 2),
            *pairs(4, 3),
            *pairs(4, 3, 2),
            *pairs(4, 3, 2),
            *pairs(4, 3),
            *pairs(7),
            *pairs(7),
            *pairs(7),
            *pairs(2),
            *pairs(4, 7),
            *pairs(7),
            *pairs(8),
        ],
        compiler_params=pltpu.CompilerParams(
            collective_id=0, has_side_effects=True, vmem_limit_bytes=60 * 1024 * 1024
        ),
    )(
        rows,
        task_ids.reshape(1, 32),
        task_embed,
        norm_gain,
        layer_weight.reshape(4, 4, 4, 2, 128, 128),
    )


def solution(mesh):
    return jax.shard_map(
        shards,
        mesh=mesh,
        in_specs=(P(("row", "col"), None), P(("row", "col")), P(), P(), P(None, None, "col")),
        out_specs=P("row", "col"),
        check_vma=False,
    )
```

```python
import functools

import jax
import jax.numpy as jnp
from jax import lax
from jax.experimental import pallas as pl
from jax.experimental.pallas import tpu as pltpu
from jax.sharding import PartitionSpec as P

MESH = pl.DeviceIdType.MESH
F32 = jnp.float32
BF16 = jnp.bfloat16
EPS = 1e-06
LAYERS = 4
CUBE = [(1, 0, 0), (0, 1, 0), (0, 0, 1), (1, 1, 0), (0, 1, 1), (1, 0, 1), (1, 1, 1)]
NEXT = (1, 2, 0)
PREV = (2, 0, 1)
THIRDS = (((0, 2), (2, 1), (3, 1)), ((4, 1), (5, 2), (7, 1)))
ROW_THIRDS = ((0, 48), (48, 48), (96, 32))
FAR = [(i // 4, (i // 2) % 2, i % 2) for i in range(1, 8)]


def flip(bit, on):
    return 1 - bit if on else bit


def kernel(
    rows_in, ids_in, embed_in, gain_in, w_ref, out_ref,
    rows_ref, ids_ref, embed_ref, gain_ref, outv,
    wv, a, act, acc, h0s, h0, gp, pm, f, idg, idf, pos, stat, invb, oacc,
    inp, outs, wl, wsend, w1r, w2r, wdr, asend, a1r, a2r, a3r, tsend, tr,
    hs, hr, i1s, i1r, i2s, i2r, i3s, i3r, fs, fr, fds, fdr,
):
    row, col = lax.axis_index("row"), lax.axis_index("col")
    xh, core = row // 2, row % 2
    z, y, x = col // 8, (col // 2) % 4, col % 2
    zh, zo, yh, yo = z // 2, z % 2, y // 2, y % 2
    zl, yl = zo + zh - 2 * zo * zh, yo + yh - 2 * yo * yh
    qme = zl * 4 + yl * 2 + x

    def cube_dev(fl):
        return (row, (zh * 2 + flip(zo, fl[2])) * 8 + (yh * 2 + flip(yo, fl[1])) * 2 + flip(x, fl[0]))

    def cube_q(fl):
        return flip(zl, fl[2]) * 4 + flip(yl, fl[1]) * 2 + flip(x, fl[0])

    def far_dev(fl):
        zz = 3 - z if fl[1] else z
        yy = 3 - y if fl[2] else y
        return (flip(xh, fl[0]) * 2 + core, zz * 8 + yy * 2 + x)

    def slot(fa, fb):
        return flip(zh, fa) * 2 + flip(yh, fb)

    def cols(s):
        return pl.ds(pl.multiple_of(s * 128, 128), 128)

    partner = (xh * 2 + (1 - core), col)
    links = [cube_dev(CUBE[d]) for d in range(3)]
    wlinks = [far_dev((0, 0, 1)), far_dev((0, 1, 0))]

    def remote(src, dst, ss, rs, dev):
        return pltpu.make_async_remote_copy(
            src_ref=src, dst_ref=dst, send_sem=ss, recv_sem=rs, device_id=dev, device_id_type=MESH
        )

    def both(ref, ss, rs, dev):
        return remote(ref, ref, ss, rs, dev)

    def arrived(ref, sem):
        both(ref, sem, sem, partner).wait_recv()

    def left(ref, sem):
        both(ref, sem, sem, partner).wait_send()

    def load_own(l):
        for zz in range(4):
            for yy in range(4):
                q0 = min(zz, 3 - zz) * 4 + min(yy, 3 - yy) * 2
                pltpu.make_async_copy(
                    w_ref.at[l, zz, yy],
                    wv.at[l, slot(0, 0), pl.ds(q0, 2), (zz // 2) * 2 + yy // 2],
                    wl.at[l],
                ).start()

    def own_loaded(l):
        whole = wv.at[l, slot(0, 0)]
        pltpu.make_async_copy(whole, whole, wl.at[l]).wait()

    def wpart(l, fa, fb, q0, n):
        return wv.at[l, slot(fa, fb), pl.ds(q0, n)]

    def w1(l, k, j):
        return both(wpart(l, 0, 0, core * 4 + 2 * j, 2), wsend.at[l], w1r.at[l, int(k != j)], wlinks[k])

    def w2(l, k):
        fa, fb = (1, 0) if k == 0 else (0, 1)
        return both(wpart(l, fa, fb, core * 4 + 2 * (1 - k), 2), wsend.at[l], w2r.at[l], wlinks[k])

    def wd(l, k):
        fa, fb = ((0, 1), (1, 0), (1, 1))[k]
        return both(wpart(l, fa, fb, core * 4, 4), wsend.at[l], wdr.at[l], partner)

    def w1_send(l):
        own_loaded(l)
        for k, j in ((0, 0), (1, 1), (0, 1), (1, 0)):
            w1(l, k, j).start()

    def w1_first(l):
        arrived(wv.at[l, 0, pl.ds(0, 4)], w1r.at[l, 0])
        w2(l, 1).start()
        w2(l, 0).start()

    def w1_rest(l):
        arrived(wv.at[l, 0, pl.ds(0, 4)], w1r.at[l, 1])
        wd(l, 0).start()
        wd(l, 1).start()

    def w2_in(l):
        arrived(wv.at[l, 0, pl.ds(0, 4)], w2r.at[l])
        wd(l, 2).start()

    def wd_in(l):
        arrived(wv.at[l, pl.ds(0, 3), pl.ds(0, 4)], wdr.at[l])

    def drain_weights(l):
        left(wv.at[l, pl.ds(0, 3)], wsend.at[l])

    def zero(l):
        return isinstance(l, int) and l == 0

    def chunk(l, fl, i):
        if zero(l):
            at = pl.ds(pl.multiple_of(flip(yo, fl[1]) * 64 + flip(x, fl[0]) * 32, 32), 32)
            return a.at[0, pl.ds(4 * i, 4), flip(zo, fl[2]), at, :]
        return a.at[l, cube_q(fl), i]

    def third(l, fl, e, i):
        if zero(l):
            at = pl.ds(pl.multiple_of(flip(yo, fl[1]) * 64 + flip(x, fl[0]) * 32, 32), 32)
            return a.at[0, pl.ds(*THIRDS[i][e]), flip(zo, fl[2]), at, :]
        return a.at[l, cube_q(fl), i, pl.ds(*ROW_THIRDS[e]), :]

    ME, ALL = (0, 0, 0), (1, 1, 1)

    def pair(d):
        e = PREV[d]
        return tuple(int(k in (d, e)) for k in range(3))

    def s1(l, d, i):
        return both(chunk(l, ME, i), asend.at[l], a1r.at[l, i], links[d])

    def s2(l, d, i):
        return both(chunk(l, CUBE[PREV[d]], i), asend.at[l], a2r.at[l, i], links[d])

    def s3(l, d, i):
        return both(third(l, pair(PREV[d]), d, i), asend.at[l], a3r.at[l, i], links[d])

    def step1(l, i):
        for d in range(3):
            s1(l, d, i).start()

    def step2(l, i):
        arrived(a.at[l, pl.ds(0, 3), 0], a1r.at[l, i])
        for d in range(3):
            s2(l, d, i).start()

    def step3(l, i):
        arrived(a.at[l, pl.ds(0, 3), 0], a2r.at[l, i])
        for d in range(3):
            s3(l, d, i).start()

    def step3_in(l, i):
        arrived(a.at[l, 0, 0], a3r.at[l, i])

    def drain_act(l):
        left(a.at[l, pl.ds(0, 7)], asend.at[l])

    def stat_copy(l, k, i):
        return both(stat.at[l, i, qme], tsend.at[l], tr.at[l, i], cube_dev(CUBE[k]))

    def drain_stats(l):
        left(stat.at[l, :, pl.ds(0, 7)], tsend.at[l])

    def eye():
        return lax.broadcasted_iota(jnp.int32, (128, 128), 0) == lax.broadcasted_iota(jnp.int32, (128, 128), 1)

    def weight(l, q):
        return jnp.concatenate([wv[l, k, q].reshape(512, 128) for k in range(4)], axis=1)

    def multiply(l, i, qs, src, first):
        total = jnp.dot(src(qs[0]), weight(l, qs[0]), preferred_element_type=F32)
        for q in qs[1:]:
            total = total + jnp.dot(src(q), weight(l, q), preferred_element_type=F32)
        acc[i] = total if first else acc[i] + total

    def finish(l, i, held):
        new = (held.astype(F32) + acc[i]).astype(BF16)
        a[l + 1, qme, i] = new
        val = new.astype(F32)
        sq = val * val
        sq = (sq[:, 0:128] + sq[:, 128:256]) + (sq[:, 256:384] + sq[:, 384:512])
        total = jnp.sum(sq, axis=1, keepdims=True)
        line = jnp.sum(jnp.where(eye(), total, 0.0), axis=0, keepdims=True)
        stat[l + 1, i, qme] = jnp.broadcast_to(line, (8, 128))

    def begin(l, i):
        for k in range(7):
            stat_copy(l, k, i).start()
        step1(l, i)

    def read_stats(l, i):
        arrived(stat.at[l, i, pl.ds(0, 7)], tr.at[l, i])
        total = stat[l, i, 0]
        for q in range(1, 8):
            total = total + stat[l, i, q]
        half = 0.5 * lax.rsqrt(total[0:1] * (1.0 / 4096.0) + EPS)
        tall = jnp.sum(jnp.where(eye(), half, 0.0), axis=1, keepdims=True)
        invb[i] = jnp.broadcast_to(tall, (128, 128))

    def activate(l, i, q):
        for t in range(4):
            c = slice(t * 128, t * 128 + 128)
            u = a[l, q, i, :, c].astype(F32) * invb[i] * gp[l, q, 0:1, c]
            act[q, i, :, c] = (u + u * jnp.tanh(u)).astype(BF16)

    def h_copy(k):
        dst = h0.at[zo, pl.ds(pl.multiple_of(yo * 64 + x * 32, 32), 32), :]
        return remote(h0s.at[cube_q(CUBE[k])], dst, hs, hr, cube_dev(CUBE[k]))

    def id1(k):
        return both(idg.at[zo, yo * 2 + x], i1s, i1r, cube_dev(CUBE[k]))

    def far_at(fl):
        return (flip(xh, fl[0]) * 2 + core) * 2 + flip(zh, fl[1]), flip(yh, fl[2])

    g_me, b_me = far_at(ME)
    seven = stat.at[0, 0, pl.ds(0, 7)]

    def id2(k):
        return remote(idg, idf.at[g_me, :, b_me], i2s, i2r, far_dev(FAR[k]))

    def id3(k):
        return both(idf.at[pl.ds((k * 2 + core) * 2, 2)], i3s, i3r, partner)

    def out1(k, i):
        src = a.at[LAYERS, qme, i, :, cols(slot(FAR[k][1], FAR[k][2]))]
        return remote(src, f.at[g_me, i, b_me], fs, fr.at[k], far_dev(FAR[k]))

    def out_begin(i):
        for k in range(7):
            out1(k, i).start()
        f[g_me, i, b_me] = a[LAYERS, qme, i, :, cols(slot(0, 0))]

    def out2(k):
        fl = ([ME] + FAR)[k]
        g, b = far_at(fl)
        return both(f.at[g, :, b], fds, fdr, partner)

    def positions():
        spread = idf[...].reshape(1024, 128).astype(F32).astype(BF16)
        k = lax.broadcasted_iota(jnp.int32, (32, 1024), 0)
        j = lax.broadcasted_iota(jnp.int32, (32, 1024), 1)
        pick = jnp.where((j // 32 == k) & (j % 8 == 0), 1.0, 0.0).astype(BF16)
        code = jnp.dot(pick, spread, preferred_element_type=F32)
        member = jnp.concatenate([jnp.where(code == 8.0 - t, 1.0, 0.0) for t in range(8)], axis=0).astype(BF16)
        i0 = lax.broadcasted_iota(jnp.int32, (128, 128), 0)
        i1 = lax.broadcasted_iota(jnp.int32, (128, 128), 1)
        upper = jnp.where(i0 < i1, 1.0, 0.0).astype(BF16)
        within = jnp.dot(member, upper, preferred_element_type=F32)
        count = jnp.dot(member, jnp.ones((128, 128), BF16), preferred_element_type=F32).astype(BF16)
        j0 = lax.broadcasted_iota(jnp.int32, (256, 256), 0)
        j1 = lax.broadcasted_iota(jnp.int32, (256, 256), 1)
        lower = jnp.where(j1 < j0, 1.0, 0.0).astype(BF16)
        place = jnp.dot(lower, count, preferred_element_type=F32) + within
        where = jnp.full((32, 128), -1.0, F32)
        for t in range(8):
            where = jnp.where(code == 8.0 - t, place[t * 32 : t * 32 + 32], where)
        for k in range(32):
            pos[k, 0:1, :] = where[k : k + 1]

    def selection(k0, k1):
        slots = (lax.broadcasted_iota(jnp.int32, (1024, 128), 0) * 4 + row).astype(F32)

        def body(k, carry):
            for half in range(2):
                hit = slots == pos[k * 2 + half, 0:1, :]
                pm[k, :, half * 128 : half * 128 + 128] = jnp.where(hit, 1.0, 0.0).astype(BF16)
            return carry

        lax.fori_loop(k0, k1, body, 0)

    barrier = pltpu.get_barrier_semaphore()
    peers = [cube_dev(fl) for fl in CUBE] + [far_dev(fl) for fl in FAR] + [partner]
    for dev in peers:
        pl.semaphore_signal(barrier, inc=1, device_id=dev, device_id_type=MESH)
    inputs = [
        pltpu.make_async_copy(src, dst, inp.at[k])
        for k, (src, dst) in enumerate(
            ((ids_in, ids_ref), (rows_in, rows_ref), (embed_in, embed_ref), (gain_in, gain_ref))
        )
    ]
    for copy in inputs:
        copy.start()
    for l in range(LAYERS):
        load_own(l)

    inputs[0].wait()
    ids = 8.0 - ids_ref[...].astype(F32)
    i0 = lax.broadcasted_iota(jnp.int32, (32, 32), 0)
    i1 = lax.broadcasted_iota(jnp.int32, (32, 32), 1)
    code = jnp.sum(jnp.where(i0 == i1, ids, 0.0), axis=1, keepdims=True)
    lane = lax.broadcasted_iota(jnp.int32, (32, 128), 1)
    sub = lax.broadcasted_iota(jnp.int32, (32, 128), 0)
    line = jnp.sum(jnp.where(lane == sub + (col % 4) * 32, code, 0.0), axis=0, keepdims=True)
    idg[zo, yo * 2 + x] = jnp.broadcast_to(line, (8, 128)).astype(jnp.int32)
    for copy in inputs[1:]:
        copy.wait()
    own_rows = pl.ds(pl.multiple_of(yo * 64 + x * 32, 32), 32)
    square = jnp.zeros((32, 128), F32)
    tiles = [
        (q, s, ((q // 4 if s < 2 else 3 - q // 4) * 8 + ((q // 2) % 2 if s % 2 == 0 else 3 - (q // 2) % 2) * 2 + q % 2) * 128)
        for q in range(8)
        for s in range(4)
    ]
    for q, s, c in tiles:
        table = embed_ref[:, c : c + 128].astype(F32)
        term = jnp.zeros((32, 128), F32)
        for t in range(8):
            term = jnp.where(code == 8.0 - t, table[t : t + 1], term)
        start = (rows_ref[:, c : c + 128].astype(F32) + term).astype(BF16)
        h0s[q, :, s * 128 : s * 128 + 128] = start
        start = start.astype(F32)
        square = square + start * start
        for l in range(LAYERS):
            gp[l, q, 0:1, s * 128 : s * 128 + 128] = gain_ref[l : l + 1, c : c + 128]
    half = 0.5 * lax.rsqrt(jnp.sum(square, axis=1, keepdims=True) * (1.0 / 4096.0) + EPS)
    for q, s, c in tiles:
        lanes = slice(s * 128, s * 128 + 128)
        u = h0s[q, :, lanes].astype(F32) * half * gp[0, q, 0:1, lanes]
        a[0, q, zo, own_rows, lanes] = (u + u * jnp.tanh(u)).astype(BF16)
    h0[zo, own_rows, :] = h0s[qme]

    pl.semaphore_wait(barrier, len(peers))
    for k in range(7):
        id1(k).start()
    step1(0, 0)
    step1(0, 1)
    w1_send(0)

    step2(0, 0)
    w1_first(0)
    w1_send(1)
    step2(0, 1)
    step3(0, 0)
    for k in range(7):
        h_copy(k).start()
    step3(0, 1)
    arrived(seven, i1r)
    idf[g_me, :, b_me] = idg[...]
    for k in range(7):
        id2(k).start()
    w1_rest(0)
    step3_in(0, 0)
    step3_in(0, 1)
    w2_in(0)
    wd_in(0)
    multiply(0, 0, range(8), lambda q: a[0, q, 0], True)
    arrived(h0s.at[pl.ds(0, 7)], hr)
    finish(0, 0, h0[0])
    begin(1, 0)
    multiply(0, 1, range(8), lambda q: a[0, q, 1], True)
    finish(0, 1, h0[1])
    begin(1, 1)

    def layer(l, carry):
        near = [cube_q(CUBE[d]) for d in range(3)]
        mid = [cube_q(pair(d)) for d in range(3)]
        w1_first(l)

        @pl.when(l < LAYERS - 1)
        def _():
            w1_send(l + 1)

        read_stats(l, 0)
        activate(l, 0, qme)
        step2(l, 0)
        read_stats(l, 1)
        activate(l, 1, qme)
        step2(l, 1)
        for q in near:
            activate(l, 0, q)
        step3(l, 0)
        for q in near:
            activate(l, 1, q)
        w1_rest(l)
        step3(l, 1)

        @pl.when(l == 1)
        def _():
            arrived(idf.at[pl.ds(0, 7), :, 0], i2r)
            for k in range(2):
                id3(k).start()
            drain_act(0)
            left(h0s.at[pl.ds(0, 7)], hs)
            left(seven, i1s)

        @pl.when(l == 2)
        def _():
            arrived(idf.at[pl.ds(0, 4)], i3r)
            positions()
            left(idf.at[pl.ds(0, 7), :, 0], i2s)

        @pl.when(l >= 2)
        def _():
            selection((l - 2) * 8, (l - 1) * 8)
            drain_act(l - 1)
            drain_stats(l - 1)

        drain_weights(l - 1)
        for q in mid:
            activate(l, 0, q)
        w2_in(l)
        for q in mid:
            activate(l, 1, q)
        wd_in(l)
        for i in range(2):
            multiply(l, i, [qme] + near + mid, lambda q: act[q, i], True)
            step3_in(l, i)
            activate(l, i, cube_q(ALL))
            multiply(l, i, [cube_q(ALL)], lambda q: act[q, i], False)
            finish(l, i, a[l, qme, i])

            @pl.when(l < LAYERS - 1)
            def _():
                begin(l + 1, i)

            @pl.when(l == LAYERS - 1)
            def _():
                out_begin(i)

        return carry

    lax.fori_loop(1, LAYERS, layer, 0)

    out2(0).start()
    drain_weights(LAYERS - 1)
    drain_act(LAYERS - 1)
    drain_stats(LAYERS - 1)
    left(idf.at[pl.ds(0, 4)], i3s)

    def place(first, last, groups):
        for m in range(4):
            lines = slice(m * 256, m * 256 + 256)
            total = None if first else oacc[lines]
            for at in groups:
                for k in range(2):
                    part = jnp.dot(
                        pm[at * 2 + k, lines], f[at, k].reshape(256, 128), preferred_element_type=F32
                    )
                    total = part if total is None else total + part
            if last:
                outv[lines] = total.astype(BF16)
                pltpu.make_async_copy(outv.at[lines], out_ref.at[lines], outs).start()
            else:
                oacc[lines] = total

    for k in range(3):
        arrived(f.at[0, :, 0], fr.at[k])
        out2(k + 1).start()
    place(True, False, [(xh * 2 + core) * 2 + k for k in range(2)])
    for k in range(3, 7):
        arrived(f.at[0, :, 0], fr.at[k])
        out2(k + 1).start()
    place(False, False, [((1 - xh) * 2 + core) * 2 + k for k in range(2)])
    arrived(f.at[pl.ds(0, 4)], fdr)
    place(False, True, [(k // 2 * 2 + 1 - core) * 2 + k % 2 for k in range(4)])
    pltpu.make_async_copy(outv, out_ref, outs).wait()

    left(f.at[pl.ds(0, 7), :, 0], fs)
    left(f.at[pl.ds(0, 4)], fds)


def shards(rows, task_ids, task_embed, norm_gain, layer_weight):
    dma = pltpu.SemaphoreType.DMA
    vmem = pltpu.VMEM
    return pl.pallas_call(
        kernel,
        out_shape=jax.ShapeDtypeStruct((1024, 128), BF16),
        in_specs=[pl.BlockSpec(memory_space=pl.ANY)] * 5,
        out_specs=pl.BlockSpec(memory_space=pl.ANY),
        scratch_shapes=[
            vmem((32, 4096), BF16),
            vmem((1, 32), jnp.int32),
            vmem((8, 4096), BF16),
            vmem((4, 4096), F32),
            vmem((1024, 128), BF16),
            vmem((4, 4, 8, 4, 128, 128), BF16),
            vmem((5, 8, 2, 128, 512), BF16),
            vmem((8, 2, 128, 512), BF16),
            vmem((2, 128, 512), F32),
            vmem((8, 32, 512), BF16),
            vmem((2, 128, 512), BF16),
            vmem((4, 8, 8, 512), F32),
            vmem((16, 1024, 256), BF16),
            vmem((8, 2, 2, 128, 128), BF16),
            vmem((2, 4, 8, 128), jnp.int32),
            vmem((8, 2, 2, 4, 8, 128), jnp.int32),
            vmem((32, 8, 128), F32),
            vmem((5, 2, 8, 8, 128), F32),
            vmem((2, 128, 128), F32),
            vmem((1024, 128), F32),
            dma((4,)),
            dma,
            dma((4,)),
            dma((4,)),
            dma((4, 2)),
            dma((4,)),
            dma((4,)),
            dma((4,)),
            dma((4, 2)),
            dma((4, 2)),
            dma((4, 2)),
            dma((4,)),
            dma((4, 2)),
            *[dma] * 8,
            dma,
            dma((7,)),
            dma,
            dma,
        ],
        compiler_params=pltpu.CompilerParams(
            collective_id=0, has_side_effects=True, vmem_limit_bytes=60 * 1024 * 1024
        ),
    )(
        rows,
        task_ids.reshape(1, 32),
        task_embed,
        norm_gain,
        layer_weight.reshape(4, 4, 4, 2, 128, 128),
    )


def solution(mesh):
    return jax.shard_map(
        shards,
        mesh=mesh,
        in_specs=(P(("row", "col"), None), P(("row", "col")), P(), P(), P(None, None, "col")),
        out_specs=P("row", "col"),
        check_vma=False,
    )
```

```python
import functools

import jax
import jax.numpy as jnp
from jax import lax
from jax.experimental import pallas as pl
from jax.experimental.pallas import tpu as pltpu
from jax.sharding import PartitionSpec as P

MESH = pl.DeviceIdType.MESH
F32 = jnp.float32
BF16 = jnp.bfloat16
EPS = 1e-06
LAYERS = 4
CUBE = [(1, 0, 0), (0, 1, 0), (0, 0, 1), (1, 1, 0), (0, 1, 1), (1, 0, 1), (1, 1, 1)]
NEXT = (1, 2, 0)
PREV = (2, 0, 1)
THIRDS = (((0, 2), (2, 1), (3, 1)), ((4, 1), (5, 2), (7, 1)))
ROW_THIRDS = ((0, 48), (48, 48), (96, 32))
FAR = [(i // 4, (i // 2) % 2, i % 2) for i in range(1, 8)]


def flip(bit, on):
    return 1 - bit if on else bit


def kernel(
    rows_in, ids_in, embed_in, gain_in, w_ref, out_ref,
    rows_ref, ids_ref, embed_ref, gain_ref,
    wv, a, act, acc, gp, pm, f, idg, idf, pos, stat, invb, oacc,
    inp, wl, wsend, w1r, w2r, wdr, asend, a1r, a2r, a3r, tsend, tr,
    i1s, i1r, i2s, i2r, i3s, i3r, fs, fr, fds, fdr,
):
    row, col = lax.axis_index("row"), lax.axis_index("col")
    xh, core = row // 2, row % 2
    z, y, x = col // 8, (col // 2) % 4, col % 2
    zh, zo, yh, yo = z // 2, z % 2, y // 2, y % 2
    zl, yl = zo + zh - 2 * zo * zh, yo + yh - 2 * yo * yh
    qme = zl * 4 + yl * 2 + x

    def cube_dev(fl):
        return (row, (zh * 2 + flip(zo, fl[2])) * 8 + (yh * 2 + flip(yo, fl[1])) * 2 + flip(x, fl[0]))

    def cube_q(fl):
        return flip(zl, fl[2]) * 4 + flip(yl, fl[1]) * 2 + flip(x, fl[0])

    def far_dev(fl):
        zz = 3 - z if fl[1] else z
        yy = 3 - y if fl[2] else y
        return (flip(xh, fl[0]) * 2 + core, zz * 8 + yy * 2 + x)

    def slot(fa, fb):
        return flip(zh, fa) * 2 + flip(yh, fb)

    def cols(s):
        return pl.ds(pl.multiple_of(s * 128, 128), 128)

    partner = (xh * 2 + (1 - core), col)
    links = [cube_dev(CUBE[d]) for d in range(3)]
    wlinks = [far_dev((0, 0, 1)), far_dev((0, 1, 0))]

    def remote(src, dst, ss, rs, dev):
        return pltpu.make_async_remote_copy(
            src_ref=src, dst_ref=dst, send_sem=ss, recv_sem=rs, device_id=dev, device_id_type=MESH
        )

    def both(ref, ss, rs, dev):
        return remote(ref, ref, ss, rs, dev)

    def arrived(ref, sem):
        both(ref, sem, sem, partner).wait_recv()

    def left(ref, sem):
        both(ref, sem, sem, partner).wait_send()

    def load_own(l):
        for zz in range(4):
            for yy in range(4):
                q0 = min(zz, 3 - zz) * 4 + min(yy, 3 - yy) * 2
                pltpu.make_async_copy(
                    w_ref.at[l, zz, yy],
                    wv.at[l, slot(0, 0), pl.ds(q0, 2), (zz // 2) * 2 + yy // 2],
                    wl.at[l],
                ).start()

    def own_loaded(l):
        whole = wv.at[l, slot(0, 0)]
        pltpu.make_async_copy(whole, whole, wl.at[l]).wait()

    def wpart(l, fa, fb, q0, n):
        return wv.at[l, slot(fa, fb), pl.ds(q0, n)]

    def w1(l, k, j):
        return both(wpart(l, 0, 0, core * 4 + 2 * j, 2), wsend.at[l], w1r.at[l, int(k != j)], wlinks[k])

    def w2(l, k):
        fa, fb = (1, 0) if k == 0 else (0, 1)
        return both(wpart(l, fa, fb, core * 4 + 2 * (1 - k), 2), wsend.at[l], w2r.at[l], wlinks[k])

    def wd(l, k):
        fa, fb = ((0, 1), (1, 0), (1, 1))[k]
        return both(wpart(l, fa, fb, core * 4, 4), wsend.at[l], wdr.at[l], partner)

    def w1_send(l):
        own_loaded(l)
        for k, j in ((0, 0), (1, 1), (0, 1), (1, 0)):
            w1(l, k, j).start()

    def w1_first(l):
        arrived(wv.at[l, 0, pl.ds(0, 4)], w1r.at[l, 0])
        w2(l, 1).start()
        w2(l, 0).start()

    def w1_rest(l):
        arrived(wv.at[l, 0, pl.ds(0, 4)], w1r.at[l, 1])
        wd(l, 0).start()
        wd(l, 1).start()

    def w2_in(l):
        arrived(wv.at[l, 0, pl.ds(0, 4)], w2r.at[l])
        wd(l, 2).start()

    def wd_in(l):
        arrived(wv.at[l, pl.ds(0, 3), pl.ds(0, 4)], wdr.at[l])

    def drain_weights(l):
        left(wv.at[l, pl.ds(0, 3)], wsend.at[l])

    def zero(l):
        return isinstance(l, int) and l == 0

    def chunk(l, fl, i):
        if zero(l):
            at = pl.ds(pl.multiple_of(flip(yo, fl[1]) * 64 + flip(x, fl[0]) * 32, 32), 32)
            return a.at[0, pl.ds(4 * i, 4), flip(zo, fl[2]), at, :]
        return a.at[l, cube_q(fl), i]

    def third(l, fl, e, i):
        if zero(l):
            at = pl.ds(pl.multiple_of(flip(yo, fl[1]) * 64 + flip(x, fl[0]) * 32, 32), 32)
            return a.at[0, pl.ds(*THIRDS[i][e]), flip(zo, fl[2]), at, :]
        return a.at[l, cube_q(fl), i, pl.ds(*ROW_THIRDS[e]), :]

    ME, ALL = (0, 0, 0), (1, 1, 1)

    def pair(d):
        e = PREV[d]
        return tuple(int(k in (d, e)) for k in range(3))

    def s1(l, d, i):
        return both(chunk(l, ME, i), asend.at[l], a1r.at[l, i], links[d])

    def s2(l, d, i):
        return both(chunk(l, CUBE[PREV[d]], i), asend.at[l], a2r.at[l, i], links[d])

    def s3(l, d, i):
        return both(third(l, pair(PREV[d]), d, i), asend.at[l], a3r.at[l, i], links[d])

    def step1(l, i):
        for d in range(3):
            s1(l, d, i).start()

    def step2(l, i):
        arrived(a.at[l, pl.ds(0, 3), 0], a1r.at[l, i])
        for d in range(3):
            s2(l, d, i).start()

    def step3(l, i):
        arrived(a.at[l, pl.ds(0, 3), 0], a2r.at[l, i])
        for d in range(3):
            s3(l, d, i).start()

    def step3_in(l, i):
        arrived(a.at[l, 0, 0], a3r.at[l, i])

    def drain_act(l):
        left(a.at[l, pl.ds(0, 7)], asend.at[l])

    def stat_copy(l, k, i):
        return both(stat.at[l, i, qme, pl.ds(0, 1)], tsend.at[l], tr.at[l, i], cube_dev(CUBE[k]))

    def drain_stats(l):
        left(stat.at[l, :, pl.ds(0, 7), pl.ds(0, 1)], tsend.at[l])

    def eye():
        return lax.broadcasted_iota(jnp.int32, (128, 128), 0) == lax.broadcasted_iota(jnp.int32, (128, 128), 1)

    def weight(l, q):
        return jnp.concatenate([wv[l, k, q].reshape(512, 128) for k in range(4)], axis=1)

    def multiply(l, i, qs, src, first):
        total = jnp.dot(src(qs[0]), weight(l, qs[0]), preferred_element_type=F32)
        for q in qs[1:]:
            total = total + jnp.dot(src(q), weight(l, q), preferred_element_type=F32)
        acc[i] = total if first else acc[i] + total

    def finish(l, i, held):
        new = (held.astype(F32) + acc[i]).astype(BF16)
        a[l + 1, qme, i] = new
        val = new.astype(F32)
        sq = val * val
        sq = (sq[:, 0:128] + sq[:, 128:256]) + (sq[:, 256:384] + sq[:, 384:512])
        total = jnp.sum(sq, axis=1, keepdims=True)
        line = jnp.sum(jnp.where(eye(), total, 0.0), axis=0, keepdims=True)
        stat[l + 1, i, qme, 0:1] = line

    def begin(l, i):
        for k in range(7):
            stat_copy(l, k, i).start()
        step1(l, i)

    def read_stats(l, i):
        arrived(stat.at[l, i, pl.ds(0, 7), pl.ds(0, 1)], tr.at[l, i])
        total = stat[l, i, 0, 0:1]
        for q in range(1, 8):
            total = total + stat[l, i, q, 0:1]
        half = 0.5 * lax.rsqrt(total * (1.0 / 4096.0) + EPS)
        tall = jnp.sum(jnp.where(eye(), half, 0.0), axis=1, keepdims=True)
        invb[i] = jnp.broadcast_to(tall, (128, 128))

    def activate(l, i, q):
        for t in range(4):
            c = slice(t * 128, t * 128 + 128)
            u = a[l, q, i, :, c].astype(F32) * invb[i] * gp[l, q, 0:1, c]
            act[q, i, :, c] = (u + u * jnp.tanh(u)).astype(BF16)

    def id1(k):
        return both(idg.at[zo, yo * 2 + x, pl.ds(0, 1)], i1s, i1r, cube_dev(CUBE[k]))

    def far_at(fl):
        return (flip(xh, fl[0]) * 2 + core) * 2 + flip(zh, fl[1]), flip(yh, fl[2])

    g_me, b_me = far_at(ME)
    seven = stat.at[0, 0, pl.ds(0, 7), pl.ds(0, 1)]

    def id2(k):
        return both(idf.at[g_me, :, b_me], i2s, i2r, far_dev(FAR[k]))

    def id3(k):
        return both(idf.at[pl.ds((k * 2 + core) * 2, 2)], i3s, i3r, partner)

    def out1(k, i):
        src = a.at[LAYERS, qme, i, :, cols(slot(FAR[k][1], FAR[k][2]))]
        return remote(src, f.at[g_me, i, b_me], fs, fr.at[k], far_dev(FAR[k]))

    def out_begin(i):
        for k in range(7):
            out1(k, i).start()
        f[g_me, i, b_me] = a[LAYERS, qme, i, :, cols(slot(0, 0))]

    def out2(k):
        fl = ([ME] + FAR)[k]
        g, b = far_at(fl)
        return both(f.at[g, :, b], fds, fdr, partner)

    def positions():
        spread = idf[...].reshape(256, 128).astype(F32).astype(BF16)
        k = lax.broadcasted_iota(jnp.int32, (32, 256), 0)
        j = lax.broadcasted_iota(jnp.int32, (32, 256), 1)
        pick = jnp.where(j == k * 8, 1.0, 0.0).astype(BF16)
        code = jnp.dot(pick, spread, preferred_element_type=F32)
        member = jnp.concatenate([jnp.where(code == 8.0 - t, 1.0, 0.0) for t in range(8)], axis=0).astype(BF16)
        i0 = lax.broadcasted_iota(jnp.int32, (128, 128), 0)
        i1 = lax.broadcasted_iota(jnp.int32, (128, 128), 1)
        upper = jnp.where(i0 < i1, 1.0, 0.0).astype(BF16)
        within = jnp.dot(member, upper, preferred_element_type=F32)
        count = jnp.dot(member, jnp.ones((128, 128), BF16), preferred_element_type=F32).astype(BF16)
        j0 = lax.broadcasted_iota(jnp.int32, (256, 256), 0)
        j1 = lax.broadcasted_iota(jnp.int32, (256, 256), 1)
        lower = jnp.where(j1 < j0, 1.0, 0.0).astype(BF16)
        place = jnp.dot(lower, count, preferred_element_type=F32) + within
        where = jnp.full((32, 128), -1.0, F32)
        for t in range(8):
            where = jnp.where(code == 8.0 - t, place[t * 32 : t * 32 + 32], where)
        for k in range(32):
            pos[k, 0:1, :] = where[k : k + 1]

    def selection(k0, k1):
        slots = (lax.broadcasted_iota(jnp.int32, (1024, 128), 0) * 4 + row).astype(F32)

        def body(k, carry):
            for half in range(2):
                hit = slots == pos[k * 2 + half, 0:1, :]
                pm[k, :, half * 128 : half * 128 + 128] = jnp.where(hit, 1.0, 0.0).astype(BF16)
            return carry

        lax.fori_loop(k0, k1, body, 0)

    barrier = pltpu.get_barrier_semaphore()
    peers = [cube_dev(fl) for fl in CUBE] + [far_dev(fl) for fl in FAR] + [partner]
    for dev in peers:
        pl.semaphore_signal(barrier, inc=1, device_id=dev, device_id_type=MESH)
    inputs = [
        pltpu.make_async_copy(src, dst, inp.at[k])
        for k, (src, dst) in enumerate(
            ((ids_in, ids_ref), (rows_in, rows_ref), (embed_in, embed_ref), (gain_in, gain_ref))
        )
    ]
    for copy in inputs:
        copy.start()
    load_own(0)
    for k in range(2):
        idf[g_me, k, b_me] = jnp.zeros((8, 128), jnp.int32)
    pl.semaphore_wait(barrier, len(peers))
    w1_send(0)
    for l in range(1, LAYERS):
        load_own(l)

    inputs[0].wait()
    ids = 8.0 - ids_ref[...].astype(F32)
    i0 = lax.broadcasted_iota(jnp.int32, (32, 32), 0)
    i1 = lax.broadcasted_iota(jnp.int32, (32, 32), 1)
    code = jnp.sum(jnp.where(i0 == i1, ids, 0.0), axis=1, keepdims=True)
    lane = lax.broadcasted_iota(jnp.int32, (32, 128), 1)
    sub = lax.broadcasted_iota(jnp.int32, (32, 128), 0)
    line = jnp.sum(jnp.where(lane == sub + (col % 4) * 32, code, 0.0), axis=0, keepdims=True)
    idg[zo, yo * 2 + x, 0:1] = line.astype(jnp.int32)
    for copy in inputs[1:]:
        copy.wait()
    own_rows = pl.ds(pl.multiple_of(yo * 64 + x * 32, 32), 32)
    square = jnp.zeros((32, 128), F32)
    for q in range(8):
        for k in range(4):
            zz = q // 4 if k < 2 else 3 - q // 4
            yy = (q // 2) % 2 if k % 2 == 0 else 3 - (q // 2) % 2
            c = (zz * 8 + yy * 2 + q % 2) * 128
            lanes = slice(k * 128, k * 128 + 128)
            table = embed_ref[:, c : c + 128].astype(F32)
            term = jnp.zeros((32, 128), F32)
            for t in range(8):
                term = jnp.where(code == 8.0 - t, table[t : t + 1], term)
            start = (rows_ref[:, c : c + 128].astype(F32) + term).astype(BF16)
            a[0, q, zo, own_rows, lanes] = start
            start = start.astype(F32)
            square = square + start * start
            for l in range(LAYERS):
                gp[l, q, 0:1, lanes] = gain_ref[l : l + 1, c : c + 128]
    step1(0, 0)
    step1(0, 1)
    total = jnp.sum(square, axis=1, keepdims=True)
    line = jnp.sum(jnp.where(lane == sub + yo * 64 + x * 32, total, 0.0), axis=0, keepdims=True)
    stat[0, zo, qme, 0:1] = line
    stat[0, 1 - zo, qme, 0:1] = jnp.zeros((1, 128), F32)
    for k in range(7):
        id1(k).start()
        stat_copy(0, k, 0).start()
        stat_copy(0, k, 1).start()

    step2(0, 0)
    w1_first(0)
    w1_send(1)
    step2(0, 1)
    step3(0, 0)
    arrived(seven, i1r)
    for k in range(2):
        idf[g_me, k, b_me, 0:1] = idg[k, 0, 0:1] + idg[k, 1, 0:1] + idg[k, 2, 0:1] + idg[k, 3, 0:1]
    for k in range(7):
        id2(k).start()
    read_stats(0, 0)
    read_stats(0, 1)
    step3(0, 1)
    w1_rest(0)

    def activate_both(q, carry):
        activate(0, 0, q)
        activate(0, 1, q)
        return carry

    step3_in(0, 0)
    lax.fori_loop(0, 4, activate_both, 0)
    w2_in(0)
    step3_in(0, 1)
    lax.fori_loop(4, 8, activate_both, 0)
    wd_in(0)
    for i in range(2):
        multiply(0, i, range(8), lambda q: act[q, i], True)
        finish(0, i, a[0, qme, i])
        begin(1, i)

    def layer(l, carry):
        near = [cube_q(CUBE[d]) for d in range(3)]
        mid = [cube_q(pair(d)) for d in range(3)]
        w1_first(l)

        @pl.when(l < LAYERS - 1)
        def _():
            w1_send(l + 1)

        read_stats(l, 0)
        activate(l, 0, qme)
        step2(l, 0)
        read_stats(l, 1)
        activate(l, 1, qme)
        step2(l, 1)
        for q in near:
            activate(l, 0, q)
        step3(l, 0)
        for q in near:
            activate(l, 1, q)
        w1_rest(l)
        step3(l, 1)

        @pl.when(l == 1)
        def _():
            arrived(idf.at[pl.ds(0, 7), :, 0], i2r)
            for k in range(2):
                id3(k).start()
            drain_act(0)
            drain_stats(0)
            left(seven, i1s)

        @pl.when(l == 2)
        def _():
            arrived(idf.at[pl.ds(0, 4)], i3r)
            positions()
            left(idf.at[pl.ds(0, 7), :, 0], i2s)

        @pl.when(l >= 2)
        def _():
            selection((l - 2) * 8, (l - 1) * 8)
            drain_act(l - 1)
            drain_stats(l - 1)

        drain_weights(l - 1)
        for q in mid:
            activate(l, 0, q)
        w2_in(l)
        for q in mid:
            activate(l, 1, q)
        wd_in(l)
        for i in range(2):
            multiply(l, i, [qme] + near + mid, lambda q: act[q, i], True)
            step3_in(l, i)
            activate(l, i, cube_q(ALL))
            multiply(l, i, [cube_q(ALL)], lambda q: act[q, i], False)
            finish(l, i, a[l, qme, i])

            @pl.when(l < LAYERS - 1)
            def _():
                begin(l + 1, i)

            @pl.when(l == LAYERS - 1)
            def _():
                out_begin(i)

        return carry

    lax.fori_loop(1, LAYERS, layer, 0)

    out2(0).start()
    drain_weights(LAYERS - 1)
    drain_act(LAYERS - 1)
    drain_stats(LAYERS - 1)
    left(idf.at[pl.ds(0, 4)], i3s)

    def place(first, last, groups):
        for m in range(4):
            lines = slice(m * 256, m * 256 + 256)
            total = None if first else oacc[lines]
            for at in groups:
                for k in range(2):
                    part = jnp.dot(
                        pm[at * 2 + k, lines], f[at, k].reshape(256, 128), preferred_element_type=F32
                    )
                    total = part if total is None else total + part
            if last:
                out_ref[lines] = total.astype(BF16)
            else:
                oacc[lines] = total

    for k in range(3):
        arrived(f.at[0, :, 0], fr.at[k])
        out2(k + 1).start()
    place(True, False, [(xh * 2 + core) * 2 + k for k in range(2)])
    for k in range(3, 7):
        arrived(f.at[0, :, 0], fr.at[k])
        out2(k + 1).start()
    place(False, False, [((1 - xh) * 2 + core) * 2 + k for k in range(2)])
    arrived(f.at[pl.ds(0, 4)], fdr)
    place(False, True, [(k // 2 * 2 + 1 - core) * 2 + k % 2 for k in range(4)])

    left(f.at[pl.ds(0, 7), :, 0], fs)
    left(f.at[pl.ds(0, 4)], fds)


def shards(rows, task_ids, task_embed, norm_gain, layer_weight):
    dma = pltpu.SemaphoreType.DMA
    vmem = pltpu.VMEM
    return pl.pallas_call(
        kernel,
        out_shape=pltpu.VMEM((1024, 128), BF16),
        in_specs=[pl.BlockSpec(memory_space=pl.ANY)] * 5,
        out_specs=pl.BlockSpec(memory_space=pltpu.VMEM),
        scratch_shapes=[
            vmem((32, 4096), BF16),
            vmem((1, 32), jnp.int32),
            vmem((8, 4096), BF16),
            vmem((4, 4096), F32),
            vmem((4, 4, 8, 4, 128, 128), BF16),
            vmem((5, 8, 2, 128, 512), BF16),
            vmem((8, 2, 128, 512), BF16),
            vmem((2, 128, 512), F32),
            vmem((4, 8, 8, 512), F32),
            vmem((16, 1024, 256), BF16),
            vmem((8, 2, 2, 128, 128), BF16),
            vmem((2, 4, 8, 128), jnp.int32),
            vmem((8, 2, 2, 8, 128), jnp.int32),
            vmem((32, 8, 128), F32),
            vmem((5, 2, 8, 8, 128), F32),
            vmem((2, 128, 128), F32),
            vmem((1024, 128), F32),
            dma((4,)),
            dma((4,)),
            dma((4,)),
            dma((4, 2)),
            dma((4,)),
            dma((4,)),
            dma((4,)),
            dma((4, 2)),
            dma((4, 2)),
            dma((4, 2)),
            dma((4,)),
            dma((4, 2)),
            *[dma] * 6,
            dma,
            dma((7,)),
            dma,
            dma,
        ],
        compiler_params=pltpu.CompilerParams(
            collective_id=0, has_side_effects=True, vmem_limit_bytes=60 * 1024 * 1024
        ),
    )(
        rows,
        task_ids.reshape(1, 32),
        task_embed,
        norm_gain,
        layer_weight.reshape(4, 4, 4, 2, 128, 128),
    )


def solution(mesh):
    return jax.shard_map(
        shards,
        mesh=mesh,
        in_specs=(P(("row", "col"), None), P(("row", "col")), P(), P(), P(None, None, "col")),
        out_specs=P("row", "col"),
        check_vma=False,
    )
```

```python
import functools

import jax
import jax.numpy as jnp
from jax import lax
from jax.experimental import pallas as pl
from jax.experimental.pallas import tpu as pltpu
from jax.sharding import PartitionSpec as P

MESH = pl.DeviceIdType.MESH
F32 = jnp.float32
BF16 = jnp.bfloat16
EPS = 1e-06
LAYERS = 4
CUBE = [(1, 0, 0), (0, 1, 0), (0, 0, 1), (1, 1, 0), (0, 1, 1), (1, 0, 1), (1, 1, 1)]
NEXT = (1, 2, 0)
PREV = (2, 0, 1)
THIRDS = (((0, 2), (2, 1), (3, 1)), ((4, 1), (5, 2), (7, 1)))
ROW_THIRDS = ((0, 48), (48, 48), (96, 32))
FAR = [(i // 4, (i // 2) % 2, i % 2) for i in range(1, 8)]


def flip(bit, on):
    return 1 - bit if on else bit


def kernel(
    rows_in, ids_in, embed_in, gain_in, w_ref, out_ref,
    rows_ref, ids_ref, embed_ref, gain_ref,
    wv, a, act, acc, gp, pm, f, idg, idf, pos, stat, invb, oacc,
    inp, wl, wsend, w1r, w2r, wdr, asend, a1r, a2r, a3r, tsend, tr,
    i1s, i1r, i2s, i2r, i3s, i3r, fs, fr, fds, fdr,
):
    row, col = lax.axis_index("row"), lax.axis_index("col")
    xh, core = row // 2, row % 2
    z, y, x = col // 8, (col // 2) % 4, col % 2
    zh, zo, yh, yo = z // 2, z % 2, y // 2, y % 2
    zl, yl = zo + zh - 2 * zo * zh, yo + yh - 2 * yo * yh
    qme = zl * 4 + yl * 2 + x

    def cube_dev(fl):
        return (row, (zh * 2 + flip(zo, fl[2])) * 8 + (yh * 2 + flip(yo, fl[1])) * 2 + flip(x, fl[0]))

    def cube_q(fl):
        return flip(zl, fl[2]) * 4 + flip(yl, fl[1]) * 2 + flip(x, fl[0])

    def far_dev(fl):
        zz = 3 - z if fl[1] else z
        yy = 3 - y if fl[2] else y
        return (flip(xh, fl[0]) * 2 + core, zz * 8 + yy * 2 + x)

    def slot(fa, fb):
        return flip(zh, fa) * 2 + flip(yh, fb)

    def cols(s):
        return pl.ds(pl.multiple_of(s * 128, 128), 128)

    partner = (xh * 2 + (1 - core), col)
    links = [cube_dev(CUBE[d]) for d in range(3)]
    wlinks = [far_dev((0, 0, 1)), far_dev((0, 1, 0))]

    def remote(src, dst, ss, rs, dev):
        return pltpu.make_async_remote_copy(
            src_ref=src, dst_ref=dst, send_sem=ss, recv_sem=rs, device_id=dev, device_id_type=MESH
        )

    def both(ref, ss, rs, dev):
        return remote(ref, ref, ss, rs, dev)

    def arrived(ref, sem):
        both(ref, sem, sem, partner).wait_recv()

    def left(ref, sem):
        both(ref, sem, sem, partner).wait_send()

    def load_own(l):
        for zz in range(4):
            for yy in range(4):
                q0 = min(zz, 3 - zz) * 4 + min(yy, 3 - yy) * 2
                pltpu.make_async_copy(
                    w_ref.at[l, zz, yy],
                    wv.at[l, slot(0, 0), pl.ds(q0, 2), (zz // 2) * 2 + yy // 2],
                    wl.at[l],
                ).start()

    def own_loaded(l):
        whole = wv.at[l, slot(0, 0)]
        pltpu.make_async_copy(whole, whole, wl.at[l]).wait()

    def wpart(l, fa, fb, q0, n):
        return wv.at[l, slot(fa, fb), pl.ds(q0, n)]

    def w1(l, k, j):
        return both(wpart(l, 0, 0, core * 4 + 2 * j, 2), wsend.at[l], w1r.at[l, int(k != j)], wlinks[k])

    def w2(l, k):
        fa, fb = (1, 0) if k == 0 else (0, 1)
        return both(wpart(l, fa, fb, core * 4 + 2 * (1 - k), 2), wsend.at[l], w2r.at[l], wlinks[k])

    def wd(l, k):
        fa, fb = ((0, 1), (1, 0), (1, 1))[k]
        return both(wpart(l, fa, fb, core * 4, 4), wsend.at[l], wdr.at[l], partner)

    def w1_send(l):
        own_loaded(l)
        for k, j in ((0, 0), (1, 1), (0, 1), (1, 0)):
            w1(l, k, j).start()

    def w1_first(l):
        arrived(wv.at[l, 0, pl.ds(0, 4)], w1r.at[l, 0])
        w2(l, 1).start()
        w2(l, 0).start()

    def w1_rest(l):
        arrived(wv.at[l, 0, pl.ds(0, 4)], w1r.at[l, 1])
        wd(l, 0).start()
        wd(l, 1).start()

    def w2_in(l):
        arrived(wv.at[l, 0, pl.ds(0, 4)], w2r.at[l])
        wd(l, 2).start()

    def wd_in(l):
        arrived(wv.at[l, pl.ds(0, 3), pl.ds(0, 4)], wdr.at[l])

    def drain_weights(l):
        left(wv.at[l, pl.ds(0, 3)], wsend.at[l])

    def zero(l):
        return isinstance(l, int) and l == 0

    def chunk(l, fl, i):
        if zero(l):
            at = pl.ds(pl.multiple_of(flip(yo, fl[1]) * 64 + flip(x, fl[0]) * 32, 32), 32)
            return a.at[0, pl.ds(4 * i, 4), flip(zo, fl[2]), at, :]
        return a.at[l, cube_q(fl), i]

    def third(l, fl, e, i):
        if zero(l):
            at = pl.ds(pl.multiple_of(flip(yo, fl[1]) * 64 + flip(x, fl[0]) * 32, 32), 32)
            return a.at[0, pl.ds(*THIRDS[i][e]), flip(zo, fl[2]), at, :]
        return a.at[l, cube_q(fl), i, pl.ds(*ROW_THIRDS[e]), :]

    ME, ALL = (0, 0, 0), (1, 1, 1)

    def pair(d):
        e = PREV[d]
        return tuple(int(k in (d, e)) for k in range(3))

    def s1(l, d, i):
        return both(chunk(l, ME, i), asend.at[l], a1r.at[l, i], links[d])

    def s2(l, d, i):
        return both(chunk(l, CUBE[PREV[d]], i), asend.at[l], a2r.at[l, i], links[d])

    def s3(l, d, i):
        return both(third(l, pair(PREV[d]), d, i), asend.at[l], a3r.at[l, i], links[d])

    def step1(l, i):
        for d in range(3):
            s1(l, d, i).start()

    def step2(l, i):
        arrived(a.at[l, pl.ds(0, 3), 0], a1r.at[l, i])
        for d in range(3):
            s2(l, d, i).start()

    def step3(l, i):
        arrived(a.at[l, pl.ds(0, 3), 0], a2r.at[l, i])
        for d in range(3):
            s3(l, d, i).start()

    def step3_in(l, i):
        arrived(a.at[l, 0, 0], a3r.at[l, i])

    def drain_act(l):
        left(a.at[l, pl.ds(0, 7)], asend.at[l])

    def stat_copy(l, k, i):
        return both(stat.at[l, i, qme, pl.ds(0, 1)], tsend.at[l], tr.at[l, i], cube_dev(CUBE[k]))

    def drain_stats(l):
        left(stat.at[l, :, pl.ds(0, 7), pl.ds(0, 1)], tsend.at[l])

    def eye():
        return lax.broadcasted_iota(jnp.int32, (128, 128), 0) == lax.broadcasted_iota(jnp.int32, (128, 128), 1)

    def weight(l, q):
        return jnp.concatenate([wv[l, k, q].reshape(512, 128) for k in range(4)], axis=1)

    def multiply(l, i, qs, first):
        total = jnp.dot(act[qs[0], i], weight(l, qs[0]), preferred_element_type=F32)
        for q in qs[1:]:
            total = total + jnp.dot(act[q, i], weight(l, q), preferred_element_type=F32)
        acc[i] = total if first else acc[i] + total

    def finish(l, i, held):
        new = (held.astype(F32) + acc[i]).astype(BF16)
        a[l + 1, qme, i] = new
        val = new.astype(F32)
        sq = val * val
        sq = (sq[:, 0:128] + sq[:, 128:256]) + (sq[:, 256:384] + sq[:, 384:512])
        total = jnp.sum(sq, axis=1, keepdims=True)
        line = jnp.sum(jnp.where(eye(), total, 0.0), axis=0, keepdims=True)
        stat[l + 1, i, qme, 0:1] = line

    def begin(l, i):
        for k in range(7):
            stat_copy(l, k, i).start()
        step1(l, i)

    def read_stats(l, i):
        arrived(stat.at[l, i, pl.ds(0, 7), pl.ds(0, 1)], tr.at[l, i])
        total = stat[l, i, 0, 0:1]
        for q in range(1, 8):
            total = total + stat[l, i, q, 0:1]
        half = 0.5 * lax.rsqrt(total * (1.0 / 4096.0) + EPS)
        tall = jnp.sum(jnp.where(eye(), half, 0.0), axis=1, keepdims=True)
        invb[i] = jnp.broadcast_to(tall, (128, 128))

    def activate(l, i, q):
        for t in range(4):
            c = slice(t * 128, t * 128 + 128)
            u = a[l, q, i, :, c].astype(F32) * invb[i] * gp[l, q, 0:1, c]
            act[q, i, :, c] = (u + u * jnp.tanh(u)).astype(BF16)

    def id1(k):
        return both(idg.at[zo, yo * 2 + x, pl.ds(0, 1)], i1s, i1r, cube_dev(CUBE[k]))

    def far_at(fl):
        return (flip(xh, fl[0]) * 2 + core) * 2 + flip(zh, fl[1]), flip(yh, fl[2])

    g_me, b_me = far_at(ME)
    seven = stat.at[0, 0, pl.ds(0, 7), pl.ds(0, 1)]

    def id2(k):
        return both(idf.at[g_me, :, b_me], i2s, i2r, far_dev(FAR[k]))

    def id3(k):
        return both(idf.at[pl.ds((k * 2 + core) * 2, 2)], i3s, i3r, partner)

    def out1(k, i):
        src = a.at[LAYERS, qme, i, :, cols(slot(FAR[k][1], FAR[k][2]))]
        return remote(src, f.at[g_me, i, b_me], fs, fr.at[k], far_dev(FAR[k]))

    def out_begin(i):
        for k in range(7):
            out1(k, i).start()
        f[g_me, i, b_me] = a[LAYERS, qme, i, :, cols(slot(0, 0))]

    def out2(k):
        fl = ([ME] + FAR)[k]
        g, b = far_at(fl)
        return both(f.at[g, :, b], fds, fdr.at[k // 4], partner)

    def positions():
        spread = idf[...].reshape(256, 128).astype(F32).astype(BF16)
        k = lax.broadcasted_iota(jnp.int32, (32, 256), 0)
        j = lax.broadcasted_iota(jnp.int32, (32, 256), 1)
        pick = jnp.where(j == k * 8, 1.0, 0.0).astype(BF16)
        code = jnp.dot(pick, spread, preferred_element_type=F32)
        member = jnp.concatenate([jnp.where(code == 8.0 - t, 1.0, 0.0) for t in range(8)], axis=0).astype(BF16)
        i0 = lax.broadcasted_iota(jnp.int32, (128, 128), 0)
        i1 = lax.broadcasted_iota(jnp.int32, (128, 128), 1)
        upper = jnp.where(i0 < i1, 1.0, 0.0).astype(BF16)
        within = jnp.dot(member, upper, preferred_element_type=F32)
        count = jnp.dot(member, jnp.ones((128, 128), BF16), preferred_element_type=F32).astype(BF16)
        j0 = lax.broadcasted_iota(jnp.int32, (256, 256), 0)
        j1 = lax.broadcasted_iota(jnp.int32, (256, 256), 1)
        lower = jnp.where(j1 < j0, 1.0, 0.0).astype(BF16)
        place = jnp.dot(lower, count, preferred_element_type=F32) + within
        where = jnp.full((32, 128), -1.0, F32)
        for t in range(8):
            where = jnp.where(code == 8.0 - t, place[t * 32 : t * 32 + 32], where)
        for k in range(32):
            pos[k, 0:1, :] = where[k : k + 1]

    def selection(k0, k1):
        slots = (lax.broadcasted_iota(jnp.int32, (1024, 128), 0) * 4 + row).astype(F32)

        def body(k, carry):
            for half in range(2):
                hit = slots == pos[k * 2 + half, 0:1, :]
                pm[k, :, half * 128 : half * 128 + 128] = jnp.where(hit, 1.0, 0.0).astype(BF16)
            return carry

        lax.fori_loop(k0, k1, body, 0)

    barrier = pltpu.get_barrier_semaphore()
    peers = [cube_dev(fl) for fl in CUBE] + [far_dev(fl) for fl in FAR] + [partner]
    for dev in peers:
        pl.semaphore_signal(barrier, inc=1, device_id=dev, device_id_type=MESH)
    inputs = [
        pltpu.make_async_copy(src, dst, inp.at[k])
        for k, (src, dst) in enumerate(
            ((ids_in, ids_ref), (rows_in, rows_ref), (embed_in, embed_ref), (gain_in, gain_ref))
        )
    ]
    for copy in inputs:
        copy.start()
    load_own(0)
    for k in range(2):
        idf[g_me, k, b_me] = jnp.zeros((8, 128), jnp.int32)
    pl.semaphore_wait(barrier, len(peers))
    w1_send(0)
    for l in range(1, LAYERS):
        load_own(l)

    inputs[0].wait()
    ids = 8.0 - ids_ref[...].astype(F32)
    i0 = lax.broadcasted_iota(jnp.int32, (32, 32), 0)
    i1 = lax.broadcasted_iota(jnp.int32, (32, 32), 1)
    code = jnp.sum(jnp.where(i0 == i1, ids, 0.0), axis=1, keepdims=True)
    lane = lax.broadcasted_iota(jnp.int32, (32, 128), 1)
    sub = lax.broadcasted_iota(jnp.int32, (32, 128), 0)
    line = jnp.sum(jnp.where(lane == sub + (col % 4) * 32, code, 0.0), axis=0, keepdims=True)
    idg[zo, yo * 2 + x, 0:1] = line.astype(jnp.int32)
    for copy in inputs[1:]:
        copy.wait()
    own_rows = pl.ds(pl.multiple_of(yo * 64 + x * 32, 32), 32)
    square = jnp.zeros((32, 128), F32)
    for q in range(8):
        for k in range(4):
            zz = q // 4 if k < 2 else 3 - q // 4
            yy = (q // 2) % 2 if k % 2 == 0 else 3 - (q // 2) % 2
            c = (zz * 8 + yy * 2 + q % 2) * 128
            lanes = slice(k * 128, k * 128 + 128)
            table = embed_ref[:, c : c + 128].astype(F32)
            term = jnp.zeros((32, 128), F32)
            for t in range(8):
                term = jnp.where(code == 8.0 - t, table[t : t + 1], term)
            start = (rows_ref[:, c : c + 128].astype(F32) + term).astype(BF16)
            a[0, q, zo, own_rows, lanes] = start
            start = start.astype(F32)
            square = square + start * start
            for l in range(LAYERS):
                gp[l, q, 0:1, lanes] = gain_ref[l : l + 1, c : c + 128]
    for k in range(7):
        id1(k).start()
    step1(0, 0)
    step1(0, 1)
    total = jnp.sum(square, axis=1, keepdims=True)
    line = jnp.sum(jnp.where(lane == sub + yo * 64 + x * 32, total, 0.0), axis=0, keepdims=True)
    stat[0, zo, qme, 0:1] = line
    stat[0, 1 - zo, qme, 0:1] = jnp.zeros((1, 128), F32)
    for k in range(7):
        stat_copy(0, k, 0).start()
        stat_copy(0, k, 1).start()

    step2(0, 0)
    arrived(seven, i1r)
    for k in range(2):
        idf[g_me, k, b_me, 0:1] = idg[k, 0, 0:1] + idg[k, 1, 0:1] + idg[k, 2, 0:1] + idg[k, 3, 0:1]
    for k in range(7):
        id2(k).start()
    w1_first(0)
    w1_send(1)
    step2(0, 1)
    step3(0, 0)
    read_stats(0, 0)
    read_stats(0, 1)
    step3(0, 1)
    w1_rest(0)

    def activate_both(q, carry):
        activate(0, 0, q)
        activate(0, 1, q)
        return carry

    step3_in(0, 0)
    lax.fori_loop(0, 4, activate_both, 0)
    arrived(idf.at[pl.ds(0, 7), :, 0], i2r)
    for k in range(2):
        id3(k).start()
    w2_in(0)
    step3_in(0, 1)
    lax.fori_loop(4, 8, activate_both, 0)
    wd_in(0)
    for i in range(2):
        multiply(0, i, range(8), True)
        finish(0, i, a[0, qme, i])
        begin(1, i)

    arrived(idf.at[pl.ds(0, 4)], i3r)
    positions()
    selection(0, 8)

    def layer(l, carry):
        near = [cube_q(CUBE[d]) for d in range(3)]
        mid = [cube_q(pair(d)) for d in range(3)]
        w1_first(l)

        @pl.when(l < LAYERS - 1)
        def _():
            w1_send(l + 1)

        read_stats(l, 0)
        activate(l, 0, qme)
        step2(l, 0)
        read_stats(l, 1)
        activate(l, 1, qme)
        step2(l, 1)
        for q in near:
            activate(l, 0, q)
        step3(l, 0)
        for q in near:
            activate(l, 1, q)
        w1_rest(l)
        step3(l, 1)

        for q in mid:
            activate(l, 0, q)
        for q in mid:
            activate(l, 1, q)
        most = [qme] + near + mid

        @pl.when(l == 1)
        def _():
            selection(8, 16)
            drain_act(0)
            left(seven, i1s)
            left(idf.at[pl.ds(0, 7), :, 0], i2s)
            left(idf.at[pl.ds(0, 4)], i3s)

        @pl.when(l >= 2)
        def _():
            drain_act(l - 1)

        w2_in(l)
        drain_stats(l - 1)
        drain_weights(l - 1)
        wd_in(l)
        for i in range(2):
            multiply(l, i, most, True)
            step3_in(l, i)
            activate(l, i, cube_q(ALL))
            multiply(l, i, [cube_q(ALL)], False)
            finish(l, i, a[l, qme, i])

            @pl.when(l < LAYERS - 1)
            def _():
                begin(l + 1, i)

            @pl.when(l == LAYERS - 1)
            def _():
                out_begin(i)

        return carry

    lax.fori_loop(1, LAYERS, layer, 0)

    out2(0).start()
    drain_weights(LAYERS - 1)
    drain_act(LAYERS - 1)
    drain_stats(LAYERS - 1)

    def place(first, last, groups):
        for m in range(4):
            lines = slice(m * 256, m * 256 + 256)
            total = None if first else oacc[lines]
            for at in groups:
                for k in range(2):
                    part = jnp.dot(
                        pm[at * 2 + k, lines], f[at, k].reshape(256, 128), preferred_element_type=F32
                    )
                    total = part if total is None else total + part
            if last:
                out_ref[lines] = total.astype(BF16)
            else:
                oacc[lines] = total

    for k in range(3):
        arrived(f.at[0, :, 0], fr.at[k])
        out2(k + 1).start()
    place(True, False, [(xh * 2 + core) * 2 + k for k in range(2)])
    arrived(f.at[pl.ds(0, 2)], fdr.at[0])
    place(False, False, [(xh * 2 + 1 - core) * 2 + k for k in range(2)])
    for k in range(3, 7):
        arrived(f.at[0, :, 0], fr.at[k])
        out2(k + 1).start()
    place(False, False, [((1 - xh) * 2 + core) * 2 + k for k in range(2)])
    arrived(f.at[pl.ds(0, 2)], fdr.at[1])
    place(False, True, [((1 - xh) * 2 + 1 - core) * 2 + k for k in range(2)])

    left(f.at[pl.ds(0, 7), :, 0], fs)
    left(f.at[pl.ds(0, 4)], fds)


def shards(rows, task_ids, task_embed, norm_gain, layer_weight):
    dma = pltpu.SemaphoreType.DMA
    vmem = pltpu.VMEM
    return pl.pallas_call(
        kernel,
        out_shape=pltpu.VMEM((1024, 128), BF16),
        in_specs=[pl.BlockSpec(memory_space=pl.ANY)] * 5,
        out_specs=pl.BlockSpec(memory_space=pltpu.VMEM),
        scratch_shapes=[
            vmem((32, 4096), BF16),
            vmem((1, 32), jnp.int32),
            vmem((8, 4096), BF16),
            vmem((4, 4096), F32),
            vmem((4, 4, 8, 4, 128, 128), BF16),
            vmem((5, 8, 2, 128, 512), BF16),
            vmem((8, 2, 128, 512), BF16),
            vmem((2, 128, 512), F32),
            vmem((4, 8, 8, 512), F32),
            vmem((16, 1024, 256), BF16),
            vmem((8, 2, 2, 128, 128), BF16),
            vmem((2, 4, 8, 128), jnp.int32),
            vmem((8, 2, 2, 8, 128), jnp.int32),
            vmem((32, 8, 128), F32),
            vmem((5, 2, 8, 8, 128), F32),
            vmem((2, 128, 128), F32),
            vmem((1024, 128), F32),
            dma((4,)),
            dma((4,)),
            dma((4,)),
            dma((4, 2)),
            dma((4,)),
            dma((4,)),
            dma((4,)),
            dma((4, 2)),
            dma((4, 2)),
            dma((4, 2)),
            dma((4,)),
            dma((4, 2)),
            *[dma] * 6,
            dma,
            dma((7,)),
            dma,
            dma((2,)),
        ],
        compiler_params=pltpu.CompilerParams(
            collective_id=0, has_side_effects=True, vmem_limit_bytes=60 * 1024 * 1024
        ),
    )(
        rows,
        task_ids.reshape(1, 32),
        task_embed,
        norm_gain,
        layer_weight.reshape(4, 4, 4, 2, 128, 128),
    )


def solution(mesh):
    return jax.shard_map(
        shards,
        mesh=mesh,
        in_specs=(P(("row", "col"), None), P(("row", "col")), P(), P(), P(None, None, "col")),
        out_specs=P("row", "col"),
        check_vma=False,
    )
```

```python
import functools

import jax
import jax.numpy as jnp
from jax import lax
from jax.experimental import pallas as pl
from jax.experimental.pallas import tpu as pltpu
from jax.sharding import PartitionSpec as P

MESH = pl.DeviceIdType.MESH
F32 = jnp.float32
BF16 = jnp.bfloat16
EPS = 1e-06
LAYERS = 4
CUBE = [(1, 0, 0), (0, 1, 0), (0, 0, 1), (1, 1, 0), (0, 1, 1), (1, 0, 1), (1, 1, 1)]
NEXT = (1, 2, 0)
PREV = (2, 0, 1)
THIRDS = (((0, 2), (2, 1), (3, 1)), ((4, 1), (5, 2), (7, 1)))
ROW_THIRDS = ((0, 48), (48, 48), (96, 32))
FAR = [(i // 4, (i // 2) % 2, i % 2) for i in range(1, 8)]


def flip(bit, on):
    return 1 - bit if on else bit


def kernel(
    rows_in, ids_in, embed_in, gain_in, w_ref, out_ref,
    rows_ref, ids_ref, embed_ref, gain_ref,
    wv, a, act, acc, gp, pm, f, idg, idf, pos, stat, invb, oacc,
    inp, wl, wsend, w1r, w2r, wdr, asend, a1r, a2r, a3r, tsend, tr,
    i1s, i1r, i2s, i2r, i3s, i3r, fs, fr, fds, fdr,
):
    row, col = lax.axis_index("row"), lax.axis_index("col")
    xh, core = row // 2, row % 2
    z, y, x = col // 8, (col // 2) % 4, col % 2
    zh, zo, yh, yo = z // 2, z % 2, y // 2, y % 2
    zl, yl = zo + zh - 2 * zo * zh, yo + yh - 2 * yo * yh
    qme = zl * 4 + yl * 2 + x

    def cube_dev(fl):
        return (row, (zh * 2 + flip(zo, fl[2])) * 8 + (yh * 2 + flip(yo, fl[1])) * 2 + flip(x, fl[0]))

    def cube_q(fl):
        return flip(zl, fl[2]) * 4 + flip(yl, fl[1]) * 2 + flip(x, fl[0])

    def far_dev(fl):
        zz = 3 - z if fl[1] else z
        yy = 3 - y if fl[2] else y
        return (flip(xh, fl[0]) * 2 + core, zz * 8 + yy * 2 + x)

    def slot(fa, fb):
        return flip(zh, fa) * 2 + flip(yh, fb)

    def cols(s):
        return pl.ds(pl.multiple_of(s * 128, 128), 128)

    partner = (xh * 2 + (1 - core), col)
    links = [cube_dev(CUBE[d]) for d in range(3)]
    wlinks = [far_dev((0, 0, 1)), far_dev((0, 1, 0))]

    def remote(src, dst, ss, rs, dev):
        return pltpu.make_async_remote_copy(
            src_ref=src, dst_ref=dst, send_sem=ss, recv_sem=rs, device_id=dev, device_id_type=MESH
        )

    def both(ref, ss, rs, dev):
        return remote(ref, ref, ss, rs, dev)

    def arrived(ref, sem):
        both(ref, sem, sem, partner).wait_recv()

    def left(ref, sem):
        both(ref, sem, sem, partner).wait_send()

    def load_own(l):
        for zz in range(4):
            for yy in range(4):
                q0 = min(zz, 3 - zz) * 4 + min(yy, 3 - yy) * 2
                pltpu.make_async_copy(
                    w_ref.at[l, zz, yy],
                    wv.at[l, slot(0, 0), pl.ds(q0, 2), (zz // 2) * 2 + yy // 2],
                    wl.at[l],
                ).start()

    def own_loaded(l):
        whole = wv.at[l, slot(0, 0)]
        pltpu.make_async_copy(whole, whole, wl.at[l]).wait()

    def wpart(l, fa, fb, q0, n):
        return wv.at[l, slot(fa, fb), pl.ds(q0, n)]

    def w1(l, k, j):
        return both(wpart(l, 0, 0, core * 4 + 2 * j, 2), wsend.at[l], w1r.at[l, int(k != j)], wlinks[k])

    def w2(l, k):
        fa, fb = (1, 0) if k == 0 else (0, 1)
        return both(wpart(l, fa, fb, core * 4 + 2 * (1 - k), 2), wsend.at[l], w2r.at[l], wlinks[k])

    def wd(l, k):
        fa, fb = ((0, 1), (1, 0), (1, 1))[k]
        return both(wpart(l, fa, fb, core * 4, 4), wsend.at[l], wdr.at[l], partner)

    def w1_send(l):
        own_loaded(l)
        for k, j in ((0, 0), (1, 1), (0, 1), (1, 0)):
            w1(l, k, j).start()

    def w1_first(l):
        arrived(wv.at[l, 0, pl.ds(0, 4)], w1r.at[l, 0])
        w2(l, 1).start()
        w2(l, 0).start()

    def w1_rest(l):
        arrived(wv.at[l, 0, pl.ds(0, 4)], w1r.at[l, 1])
        wd(l, 0).start()
        wd(l, 1).start()

    def w2_in(l):
        arrived(wv.at[l, 0, pl.ds(0, 4)], w2r.at[l])
        wd(l, 2).start()

    def wd_in(l):
        arrived(wv.at[l, pl.ds(0, 3), pl.ds(0, 4)], wdr.at[l])

    def drain_weights(l):
        left(wv.at[l, pl.ds(0, 3)], wsend.at[l])

    def zero(l):
        return isinstance(l, int) and l == 0

    def chunk(l, fl, i):
        if zero(l):
            at = pl.ds(pl.multiple_of(flip(yo, fl[1]) * 64 + flip(x, fl[0]) * 32, 32), 32)
            return a.at[0, pl.ds(4 * i, 4), flip(zo, fl[2]), at, :]
        return a.at[l, cube_q(fl), i]

    def third(l, fl, e, i):
        if zero(l):
            at = pl.ds(pl.multiple_of(flip(yo, fl[1]) * 64 + flip(x, fl[0]) * 32, 32), 32)
            return a.at[0, pl.ds(*THIRDS[i][e]), flip(zo, fl[2]), at, :]
        return a.at[l, cube_q(fl), i, pl.ds(*ROW_THIRDS[e]), :]

    ME, ALL = (0, 0, 0), (1, 1, 1)

    def pair(d):
        e = PREV[d]
        return tuple(int(k in (d, e)) for k in range(3))

    def s1(l, d, i):
        return both(chunk(l, ME, i), asend.at[l], a1r.at[l, i], links[d])

    def s2(l, d, i):
        return both(chunk(l, CUBE[PREV[d]], i), asend.at[l], a2r.at[l, i], links[d])

    def s3(l, d, i):
        return both(third(l, pair(PREV[d]), d, i), asend.at[l], a3r.at[l, i], links[d])

    def step1(l, i):
        for d in range(3):
            s1(l, d, i).start()

    def step2(l, i):
        arrived(a.at[l, pl.ds(0, 3), 0], a1r.at[l, i])
        for d in range(3):
            s2(l, d, i).start()

    def step3(l, i):
        arrived(a.at[l, pl.ds(0, 3), 0], a2r.at[l, i])
        for d in range(3):
            s3(l, d, i).start()

    def step3_in(l, i):
        arrived(a.at[l, 0, 0], a3r.at[l, i])

    def drain_act(l):
        left(a.at[l, pl.ds(0, 7)], asend.at[l])

    def stat_copy(l, k, i):
        return both(stat.at[l, i, qme, pl.ds(0, 1)], tsend.at[l], tr.at[l, i], cube_dev(CUBE[k]))

    def drain_stats(l):
        left(stat.at[l, :, pl.ds(0, 7), pl.ds(0, 1)], tsend.at[l])

    def eye():
        return lax.broadcasted_iota(jnp.int32, (128, 128), 0) == lax.broadcasted_iota(jnp.int32, (128, 128), 1)

    def weight(l, q):
        return jnp.concatenate([wv[l, k, q].reshape(512, 128) for k in range(4)], axis=1)

    def multiply(l, i, qs, first):
        total = jnp.dot(act[qs[0], i], weight(l, qs[0]), preferred_element_type=F32)
        for q in qs[1:]:
            total = total + jnp.dot(act[q, i], weight(l, q), preferred_element_type=F32)
        acc[i] = total if first else acc[i] + total

    def finish(l, i, held):
        new = (held.astype(F32) + acc[i]).astype(BF16)
        a[l + 1, qme, i] = new

    def tell(l, i):
        val = a[l, qme, i].astype(F32)
        sq = val * val
        sq = (sq[:, 0:128] + sq[:, 128:256]) + (sq[:, 256:384] + sq[:, 384:512])
        total = jnp.sum(sq, axis=1, keepdims=True)
        line = jnp.sum(jnp.where(eye(), total, 0.0), axis=0, keepdims=True)
        stat[l, i, qme, 0:1] = line

    def begin(l, i):
        tell(l, i)
        for k in range(7):
            stat_copy(l, k, i).start()
        step1(l, i)

    def read_stats(l, i):
        arrived(stat.at[l, i, pl.ds(0, 7), pl.ds(0, 1)], tr.at[l, i])
        total = stat[l, i, 0, 0:1]
        for q in range(1, 8):
            total = total + stat[l, i, q, 0:1]
        half = 0.5 * lax.rsqrt(total * (1.0 / 4096.0) + EPS)
        tall = jnp.sum(jnp.where(eye(), half, 0.0), axis=1, keepdims=True)
        invb[i] = jnp.broadcast_to(tall, (128, 128))

    def activate(l, i, q):
        for t in range(4):
            c = slice(t * 128, t * 128 + 128)
            u = a[l, q, i, :, c].astype(F32) * invb[i] * gp[l, q, 0:1, c]
            act[q, i, :, c] = (u + u * jnp.tanh(u)).astype(BF16)

    def id1(k):
        return both(idg.at[zo, yo * 2 + x, pl.ds(0, 1)], i1s, i1r, cube_dev(CUBE[k]))

    def far_at(fl):
        return (flip(xh, fl[0]) * 2 + core) * 2 + flip(zh, fl[1]), flip(yh, fl[2])

    g_me, b_me = far_at(ME)
    seven = stat.at[0, 0, pl.ds(0, 7), pl.ds(0, 1)]

    def id2(k):
        return both(idf.at[g_me, :, b_me], i2s, i2r, far_dev(FAR[k]))

    def id3(k):
        return both(idf.at[pl.ds((k * 2 + core) * 2, 2)], i3s, i3r, partner)

    def out1(k, i):
        src = a.at[LAYERS, qme, i, :, cols(slot(FAR[k][1], FAR[k][2]))]
        return remote(src, f.at[g_me, i, b_me], fs, fr.at[k], far_dev(FAR[k]))

    def out_begin(i):
        f[g_me, i, b_me] = a[LAYERS, qme, i, :, cols(slot(0, 0))]
        for k in range(7):
            out1(k, i).start()

    def out2(k):
        fl = ([ME] + FAR)[k]
        g, b = far_at(fl)
        return both(f.at[g, :, b], fds, fdr.at[max(k // 2 - 1, 0)], partner)

    def positions():
        spread = idf[...].reshape(256, 128).astype(F32).astype(BF16)
        k = lax.broadcasted_iota(jnp.int32, (32, 256), 0)
        j = lax.broadcasted_iota(jnp.int32, (32, 256), 1)
        pick = jnp.where(j == k * 8, 1.0, 0.0).astype(BF16)
        code = jnp.dot(pick, spread, preferred_element_type=F32)
        member = jnp.concatenate([jnp.where(code == 8.0 - t, 1.0, 0.0) for t in range(8)], axis=0).astype(BF16)
        i0 = lax.broadcasted_iota(jnp.int32, (128, 128), 0)
        i1 = lax.broadcasted_iota(jnp.int32, (128, 128), 1)
        upper = jnp.where(i0 < i1, 1.0, 0.0).astype(BF16)
        within = jnp.dot(member, upper, preferred_element_type=F32)
        count = jnp.dot(member, jnp.ones((128, 128), BF16), preferred_element_type=F32).astype(BF16)
        j0 = lax.broadcasted_iota(jnp.int32, (256, 256), 0)
        j1 = lax.broadcasted_iota(jnp.int32, (256, 256), 1)
        lower = jnp.where(j1 < j0, 1.0, 0.0).astype(BF16)
        place = jnp.dot(lower, count, preferred_element_type=F32) + within
        where = jnp.full((32, 128), -1.0, F32)
        for t in range(8):
            where = jnp.where(code == 8.0 - t, place[t * 32 : t * 32 + 32], where)
        for k in range(32):
            pos[k, 0:1, :] = where[k : k + 1]

    def selection(k0, k1):
        slots = (lax.broadcasted_iota(jnp.int32, (1024, 128), 0) * 4 + row).astype(F32)

        def body(k, carry):
            for half in range(2):
                hit = slots == pos[k * 2 + half, 0:1, :]
                pm[k, :, half * 128 : half * 128 + 128] = jnp.where(hit, 1.0, 0.0).astype(BF16)
            return carry

        lax.fori_loop(k0, k1, body, 0)

    barrier = pltpu.get_barrier_semaphore()
    peers = [cube_dev(fl) for fl in CUBE] + [far_dev(fl) for fl in FAR] + [partner]
    for dev in peers:
        pl.semaphore_signal(barrier, inc=1, device_id=dev, device_id_type=MESH)
    inputs = [
        pltpu.make_async_copy(src, dst, inp.at[k])
        for k, (src, dst) in enumerate(
            ((ids_in, ids_ref), (rows_in, rows_ref), (embed_in, embed_ref), (gain_in, gain_ref))
        )
    ]
    for copy in inputs:
        copy.start()
    load_own(0)
    for k in range(2):
        idf[g_me, k, b_me] = jnp.zeros((8, 128), jnp.int32)
    pl.semaphore_wait(barrier, len(peers))
    w1_send(0)
    for l in range(1, LAYERS):
        load_own(l)

    inputs[0].wait()
    ids = 8.0 - ids_ref[...].astype(F32)
    i0 = lax.broadcasted_iota(jnp.int32, (32, 32), 0)
    i1 = lax.broadcasted_iota(jnp.int32, (32, 32), 1)
    code = jnp.sum(jnp.where(i0 == i1, ids, 0.0), axis=1, keepdims=True)
    lane = lax.broadcasted_iota(jnp.int32, (32, 128), 1)
    sub = lax.broadcasted_iota(jnp.int32, (32, 128), 0)
    line = jnp.sum(jnp.where(lane == sub + (col % 4) * 32, code, 0.0), axis=0, keepdims=True)
    idg[zo, yo * 2 + x, 0:1] = line.astype(jnp.int32)
    for copy in inputs[1:]:
        copy.wait()
    own_rows = pl.ds(pl.multiple_of(yo * 64 + x * 32, 32), 32)
    square = jnp.zeros((32, 128), F32)
    for q in range(8):
        for k in range(4):
            zz = q // 4 if k < 2 else 3 - q // 4
            yy = (q // 2) % 2 if k % 2 == 0 else 3 - (q // 2) % 2
            c = (zz * 8 + yy * 2 + q % 2) * 128
            lanes = slice(k * 128, k * 128 + 128)
            table = embed_ref[:, c : c + 128].astype(F32)
            term = jnp.zeros((32, 128), F32)
            for t in range(8):
                term = jnp.where(code == 8.0 - t, table[t : t + 1], term)
            start = (rows_ref[:, c : c + 128].astype(F32) + term).astype(BF16)
            a[0, q, zo, own_rows, lanes] = start
            start = start.astype(F32)
            square = square + start * start
            for l in range(LAYERS):
                gp[l, q, 0:1, lanes] = gain_ref[l : l + 1, c : c + 128]
    for k in range(7):
        id1(k).start()
    step1(0, 0)
    step1(0, 1)
    total = jnp.sum(square, axis=1, keepdims=True)
    line = jnp.sum(jnp.where(lane == sub + yo * 64 + x * 32, total, 0.0), axis=0, keepdims=True)
    stat[0, zo, qme, 0:1] = line
    stat[0, 1 - zo, qme, 0:1] = jnp.zeros((1, 128), F32)
    for k in range(7):
        stat_copy(0, k, 0).start()
        stat_copy(0, k, 1).start()

    step2(0, 0)
    arrived(seven, i1r)
    for k in range(2):
        idf[g_me, k, b_me, 0:1] = idg[k, 0, 0:1] + idg[k, 1, 0:1] + idg[k, 2, 0:1] + idg[k, 3, 0:1]
    for k in range(7):
        id2(k).start()
    w1_first(0)
    w1_send(1)
    step2(0, 1)
    step3(0, 0)
    read_stats(0, 0)
    read_stats(0, 1)
    step3(0, 1)
    w1_rest(0)

    def activate_both(q, carry):
        activate(0, 0, q)
        activate(0, 1, q)
        return carry

    step3_in(0, 0)
    lax.fori_loop(0, 4, activate_both, 0)
    arrived(idf.at[pl.ds(0, 7), :, 0], i2r)
    for k in range(2):
        id3(k).start()
    step3_in(0, 1)
    lax.fori_loop(4, 8, activate_both, 0)
    w2_in(0)
    wd_in(0)
    for i in range(2):
        multiply(0, i, range(8), True)
        finish(0, i, a[0, qme, i])
        begin(1, i)

    arrived(idf.at[pl.ds(0, 4)], i3r)
    positions()
    selection(0, 8)

    def layer(l, carry):
        near = [cube_q(CUBE[d]) for d in range(3)]
        mid = [cube_q(pair(d)) for d in range(3)]
        w1_first(l)

        @pl.when(l < LAYERS - 1)
        def _():
            w1_send(l + 1)

        read_stats(l, 0)
        activate(l, 0, qme)
        step2(l, 0)
        read_stats(l, 1)
        activate(l, 1, qme)
        step2(l, 1)
        for q in near:
            activate(l, 0, q)
        step3(l, 0)
        for q in near:
            activate(l, 1, q)
        w1_rest(l)
        step3(l, 1)

        for q in mid:
            activate(l, 0, q)
        for q in mid:
            activate(l, 1, q)
        most = [qme] + near + mid

        @pl.when(l == 1)
        def _():
            selection(8, 16)
            drain_act(0)
            left(seven, i1s)
            left(idf.at[pl.ds(0, 7), :, 0], i2s)
            left(idf.at[pl.ds(0, 4)], i3s)

        @pl.when(l >= 2)
        def _():
            drain_act(l - 1)

        w2_in(l)
        drain_stats(l - 1)
        drain_weights(l - 1)
        wd_in(l)
        for i in range(2):
            multiply(l, i, most, True)
            step3_in(l, i)
            activate(l, i, cube_q(ALL))
            multiply(l, i, [cube_q(ALL)], False)
            finish(l, i, a[l, qme, i])

            @pl.when(l < LAYERS - 1)
            def _():
                begin(l + 1, i)

            @pl.when(l == LAYERS - 1)
            def _():
                out_begin(i)

        return carry

    lax.fori_loop(1, LAYERS, layer, 0)

    out2(0).start()
    drain_weights(LAYERS - 1)
    drain_act(LAYERS - 1)
    drain_stats(LAYERS - 1)

    def place(first, last, groups):
        for m in range(4):
            lines = slice(m * 256, m * 256 + 256)
            total = None
            for at in groups:
                for k in range(2):
                    part = jnp.dot(
                        pm[at * 2 + k, lines], f[at, k].reshape(256, 128), preferred_element_type=F32
                    )
                    total = part if total is None else total + part
            if not first:
                total = total + oacc[lines]
            if last:
                out_ref[lines] = total.astype(BF16)
            else:
                oacc[lines] = total

    for k in range(3):
        arrived(f.at[0, :, 0], fr.at[k])
        out2(k + 1).start()
    place(True, False, [(xh * 2 + core) * 2 + k for k in range(2)])
    arrived(f.at[pl.ds(0, 2)], fdr.at[0])
    place(False, False, [(xh * 2 + 1 - core) * 2 + k for k in range(2)])
    for k in range(3, 7):
        arrived(f.at[0, :, 0], fr.at[k])
        out2(k + 1).start()
    place(False, False, [((1 - xh) * 2 + core) * 2 + k for k in range(2)])
    arrived(f.at[0], fdr.at[1])
    place(False, False, [((1 - xh) * 2 + 1 - core) * 2 + zh])
    arrived(f.at[0], fdr.at[2])
    place(False, True, [((1 - xh) * 2 + 1 - core) * 2 + 1 - zh])

    left(f.at[pl.ds(0, 7), :, 0], fs)
    left(f.at[pl.ds(0, 4)], fds)


def shards(rows, task_ids, task_embed, norm_gain, layer_weight):
    dma = pltpu.SemaphoreType.DMA
    vmem = pltpu.VMEM
    return pl.pallas_call(
        kernel,
        out_shape=pltpu.VMEM((1024, 128), BF16),
        in_specs=[pl.BlockSpec(memory_space=pl.ANY)] * 5,
        out_specs=pl.BlockSpec(memory_space=pltpu.VMEM),
        scratch_shapes=[
            vmem((32, 4096), BF16),
            vmem((1, 32), jnp.int32),
            vmem((8, 4096), BF16),
            vmem((4, 4096), F32),
            vmem((4, 4, 8, 4, 128, 128), BF16),
            vmem((5, 8, 2, 128, 512), BF16),
            vmem((8, 2, 128, 512), BF16),
            vmem((2, 128, 512), F32),
            vmem((4, 8, 8, 512), F32),
            vmem((16, 1024, 256), BF16),
            vmem((8, 2, 2, 128, 128), BF16),
            vmem((2, 4, 8, 128), jnp.int32),
            vmem((8, 2, 2, 8, 128), jnp.int32),
            vmem((32, 8, 128), F32),
            vmem((5, 2, 8, 8, 128), F32),
            vmem((2, 128, 128), F32),
            vmem((1024, 128), F32),
            dma((4,)),
            dma((4,)),
            dma((4,)),
            dma((4, 2)),
            dma((4,)),
            dma((4,)),
            dma((4,)),
            dma((4, 2)),
            dma((4, 2)),
            dma((4, 2)),
            dma((4,)),
            dma((4, 2)),
            *[dma] * 6,
            dma,
            dma((7,)),
            dma,
            dma((3,)),
        ],
        compiler_params=pltpu.CompilerParams(
            collective_id=0, has_side_effects=True, vmem_limit_bytes=60 * 1024 * 1024
        ),
    )(
        rows,
        task_ids.reshape(1, 32),
        task_embed,
        norm_gain,
        layer_weight.reshape(4, 4, 4, 2, 128, 128),
    )


def solution(mesh):
    return jax.shard_map(
        shards,
        mesh=mesh,
        in_specs=(P(("row", "col"), None), P(("row", "col")), P(), P(), P(None, None, "col")),
        out_specs=P("row", "col"),
        check_vma=False,
    )
```

```python
import functools

import jax
import jax.numpy as jnp
from jax import lax
from jax.experimental import pallas as pl
from jax.experimental.pallas import tpu as pltpu
from jax.sharding import PartitionSpec as P

MESH = pl.DeviceIdType.MESH
F32 = jnp.float32
BF16 = jnp.bfloat16
EPS = 1e-06
LAYERS = 4
CUBE = [(1, 0, 0), (0, 1, 0), (0, 0, 1), (1, 1, 0), (0, 1, 1), (1, 0, 1), (1, 1, 1)]
NEXT = (1, 2, 0)
PREV = (2, 0, 1)
THIRDS = (((0, 2), (2, 1), (3, 1)), ((4, 1), (5, 2), (7, 1)))
ROW_THIRDS = ((0, 48), (48, 48), (96, 32))
FAR = [(i // 4, (i // 2) % 2, i % 2) for i in range(1, 8)]


def flip(bit, on):
    return 1 - bit if on else bit


def kernel(
    rows_in, ids_in, embed_in, gain_in, w_ref, out_ref,
    rows_ref, ids_ref, embed_ref, gain_ref,
    wv, a, act, acc, gp, pm, f, idg, idf, pos, stat, invb, oacc,
    inp, wl, wsend, w1r, w2r, wdr, asend, a1r, a2r, a3r, tsend, tr,
    i1s, i1r, i2s, i2r, i3s, i3r, fs, fr, fds, fdr,
):
    row, col = lax.axis_index("row"), lax.axis_index("col")
    xh, core = row // 2, row % 2
    z, y, x = col // 8, (col // 2) % 4, col % 2
    zh, zo, yh, yo = z // 2, z % 2, y // 2, y % 2
    zl, yl = zo + zh - 2 * zo * zh, yo + yh - 2 * yo * yh
    qme = zl * 4 + yl * 2 + x

    def cube_dev(fl):
        return (row, (zh * 2 + flip(zo, fl[2])) * 8 + (yh * 2 + flip(yo, fl[1])) * 2 + flip(x, fl[0]))

    def cube_q(fl):
        return flip(zl, fl[2]) * 4 + flip(yl, fl[1]) * 2 + flip(x, fl[0])

    def far_dev(fl):
        zz = 3 - z if fl[1] else z
        yy = 3 - y if fl[2] else y
        return (flip(xh, fl[0]) * 2 + core, zz * 8 + yy * 2 + x)

    def slot(fa, fb):
        return flip(zh, fa) * 2 + flip(yh, fb)

    def cols(s):
        return pl.ds(pl.multiple_of(s * 128, 128), 128)

    partner = (xh * 2 + (1 - core), col)
    links = [cube_dev(CUBE[d]) for d in range(3)]
    wlinks = [far_dev((0, 0, 1)), far_dev((0, 1, 0))]

    def remote(src, dst, ss, rs, dev):
        return pltpu.make_async_remote_copy(
            src_ref=src, dst_ref=dst, send_sem=ss, recv_sem=rs, device_id=dev, device_id_type=MESH
        )

    def both(ref, ss, rs, dev):
        return remote(ref, ref, ss, rs, dev)

    def arrived(ref, sem):
        both(ref, sem, sem, partner).wait_recv()

    def left(ref, sem):
        both(ref, sem, sem, partner).wait_send()

    def load_own(l):
        for zz in range(4):
            for yy in range(4):
                q0 = min(zz, 3 - zz) * 4 + min(yy, 3 - yy) * 2
                pltpu.make_async_copy(
                    w_ref.at[l, zz, yy],
                    wv.at[l, slot(0, 0), pl.ds(q0, 2), (zz // 2) * 2 + yy // 2],
                    wl.at[l],
                ).start()

    def own_loaded(l):
        whole = wv.at[l, slot(0, 0)]
        pltpu.make_async_copy(whole, whole, wl.at[l]).wait()

    def wpart(l, fa, fb, q0, n):
        return wv.at[l, slot(fa, fb), pl.ds(q0, n)]

    def w1(l, k, j):
        return both(wpart(l, 0, 0, core * 4 + 2 * j, 2), wsend.at[l], w1r.at[l, int(k != j)], wlinks[k])

    def w2(l, k):
        fa, fb = (1, 0) if k == 0 else (0, 1)
        return both(wpart(l, fa, fb, core * 4 + 2 * (1 - k), 2), wsend.at[l], w2r.at[l], wlinks[k])

    def wd(l, k):
        fa, fb = ((0, 1), (1, 0), (1, 1))[k]
        return both(wpart(l, fa, fb, core * 4, 4), wsend.at[l], wdr.at[l], partner)

    def w1_send(l):
        own_loaded(l)
        for k, j in ((0, 0), (1, 1), (0, 1), (1, 0)):
            w1(l, k, j).start()

    def w1_first(l):
        arrived(wv.at[l, 0, pl.ds(0, 4)], w1r.at[l, 0])
        w2(l, 1).start()
        w2(l, 0).start()

    def w1_rest(l):
        arrived(wv.at[l, 0, pl.ds(0, 4)], w1r.at[l, 1])
        wd(l, 0).start()
        wd(l, 1).start()

    def w2_in(l):
        arrived(wv.at[l, 0, pl.ds(0, 4)], w2r.at[l])
        wd(l, 2).start()

    def wd_in(l):
        arrived(wv.at[l, pl.ds(0, 3), pl.ds(0, 4)], wdr.at[l])

    def drain_weights(l):
        left(wv.at[l, pl.ds(0, 3)], wsend.at[l])

    def zero(l):
        return isinstance(l, int) and l == 0

    def chunk(l, fl, i):
        if zero(l):
            at = pl.ds(pl.multiple_of(flip(yo, fl[1]) * 64 + flip(x, fl[0]) * 32, 32), 32)
            return a.at[0, pl.ds(4 * i, 4), flip(zo, fl[2]), at, :]
        return a.at[l, cube_q(fl), i]

    def third(l, fl, e, i):
        if zero(l):
            at = pl.ds(pl.multiple_of(flip(yo, fl[1]) * 64 + flip(x, fl[0]) * 32, 32), 32)
            return a.at[0, pl.ds(*THIRDS[i][e]), flip(zo, fl[2]), at, :]
        return a.at[l, cube_q(fl), i, pl.ds(*ROW_THIRDS[e]), :]

    ME, ALL = (0, 0, 0), (1, 1, 1)

    def pair(d):
        e = PREV[d]
        return tuple(int(k in (d, e)) for k in range(3))

    def s1(l, d, i):
        return both(chunk(l, ME, i), asend.at[l], a1r.at[l, i], links[d])

    def s2(l, d, i):
        return both(chunk(l, CUBE[PREV[d]], i), asend.at[l], a2r.at[l, i], links[d])

    def s3(l, d, i):
        return both(third(l, pair(PREV[d]), d, i), asend.at[l], a3r.at[l, i], links[d])

    def step1(l, i):
        for d in range(3):
            s1(l, d, i).start()

    def step2(l, i):
        arrived(a.at[l, pl.ds(0, 3), 0], a1r.at[l, i])
        for d in range(3):
            s2(l, d, i).start()

    def step3(l, i):
        arrived(a.at[l, pl.ds(0, 3), 0], a2r.at[l, i])
        for d in range(3):
            s3(l, d, i).start()

    def step3_in(l, i):
        arrived(a.at[l, 0, 0], a3r.at[l, i])

    def drain_act(l):
        left(a.at[l, pl.ds(0, 7)], asend.at[l])

    def stat_copy(l, k, i):
        return both(stat.at[l, i, qme, pl.ds(0, 1)], tsend.at[l], tr.at[l, i], cube_dev(CUBE[k]))

    def drain_stats(l):
        left(stat.at[l, :, pl.ds(0, 7), pl.ds(0, 1)], tsend.at[l])

    def eye():
        return lax.broadcasted_iota(jnp.int32, (128, 128), 0) == lax.broadcasted_iota(jnp.int32, (128, 128), 1)

    def weight(l, q):
        return jnp.concatenate([wv[l, k, q].reshape(512, 128) for k in range(4)], axis=1)

    def multiply(l, i, qs, first):
        total = jnp.dot(act[qs[0], i], weight(l, qs[0]), preferred_element_type=F32)
        for q in qs[1:]:
            total = total + jnp.dot(act[q, i], weight(l, q), preferred_element_type=F32)
        acc[i] = total if first else acc[i] + total

    def finish(l, i, held):
        new = (held.astype(F32) + acc[i]).astype(BF16)
        a[l + 1, qme, i] = new

    def tell(l, i):
        val = a[l, qme, i].astype(F32)
        sq = val * val
        sq = (sq[:, 0:128] + sq[:, 128:256]) + (sq[:, 256:384] + sq[:, 384:512])
        total = jnp.sum(sq, axis=1, keepdims=True)
        line = jnp.sum(jnp.where(eye(), total, 0.0), axis=0, keepdims=True)
        stat[l, i, qme, 0:1] = line

    def begin(l, i):
        tell(l, i)
        for k in range(7):
            stat_copy(l, k, i).start()
        step1(l, i)

    def read_stats(l, i):
        arrived(stat.at[l, i, pl.ds(0, 7), pl.ds(0, 1)], tr.at[l, i])
        total = stat[l, i, 0, 0:1]
        for q in range(1, 8):
            total = total + stat[l, i, q, 0:1]
        half = 0.5 * lax.rsqrt(total * (1.0 / 4096.0) + EPS)
        tall = jnp.sum(jnp.where(eye(), half, 0.0), axis=1, keepdims=True)
        invb[i] = jnp.broadcast_to(tall, (128, 128))

    def activate(l, i, q):
        for t in range(4):
            c = slice(t * 128, t * 128 + 128)
            u = a[l, q, i, :, c].astype(F32) * invb[i] * gp[l, q, 0:1, c]
            act[q, i, :, c] = (u + u * jnp.tanh(u)).astype(BF16)

    def id1(k):
        return both(idg.at[zo, yo * 2 + x, pl.ds(0, 1)], i1s, i1r, cube_dev(CUBE[k]))

    def far_at(fl):
        return (flip(xh, fl[0]) * 2 + core) * 2 + flip(zh, fl[1]), flip(yh, fl[2])

    g_me, b_me = far_at(ME)
    seven = stat.at[0, 0, pl.ds(0, 7), pl.ds(0, 1)]

    def id2(k):
        return both(idf.at[g_me, :, b_me], i2s, i2r, far_dev(FAR[k]))

    def id3(k):
        return both(idf.at[pl.ds((k * 2 + core) * 2, 2)], i3s, i3r, partner)

    def out1(k, i):
        src = a.at[LAYERS, qme, i, :, cols(slot(FAR[k][1], FAR[k][2]))]
        return remote(src, f.at[g_me, i, b_me], fs, fr.at[k], far_dev(FAR[k]))

    def out_begin(i):
        f[g_me, i, b_me] = a[LAYERS, qme, i, :, cols(slot(0, 0))]
        for k in range(7):
            out1(k, i).start()

    def out2(k):
        fl = ([ME] + FAR)[k]
        g, b = far_at(fl)
        return both(f.at[g, :, b], fds, fdr.at[max(k // 2 - 1, 0)], partner)

    def positions():
        spread = idf[...].reshape(256, 128).astype(F32).astype(BF16)
        k = lax.broadcasted_iota(jnp.int32, (32, 256), 0)
        j = lax.broadcasted_iota(jnp.int32, (32, 256), 1)
        pick = jnp.where(j == k * 8, 1.0, 0.0).astype(BF16)
        code = jnp.dot(pick, spread, preferred_element_type=F32)
        member = jnp.concatenate([jnp.where(code == 8.0 - t, 1.0, 0.0) for t in range(8)], axis=0).astype(BF16)
        i0 = lax.broadcasted_iota(jnp.int32, (128, 128), 0)
        i1 = lax.broadcasted_iota(jnp.int32, (128, 128), 1)
        upper = jnp.where(i0 < i1, 1.0, 0.0).astype(BF16)
        within = jnp.dot(member, upper, preferred_element_type=F32)
        count = jnp.dot(member, jnp.ones((128, 128), BF16), preferred_element_type=F32).astype(BF16)
        j0 = lax.broadcasted_iota(jnp.int32, (256, 256), 0)
        j1 = lax.broadcasted_iota(jnp.int32, (256, 256), 1)
        lower = jnp.where(j1 < j0, 1.0, 0.0).astype(BF16)
        place = jnp.dot(lower, count, preferred_element_type=F32) + within
        where = jnp.full((32, 128), -1.0, F32)
        for t in range(8):
            where = jnp.where(code == 8.0 - t, place[t * 32 : t * 32 + 32], where)
        for k in range(32):
            pos[k, 0:1, :] = where[k : k + 1]

    def selection(k0, k1):
        slots = (lax.broadcasted_iota(jnp.int32, (1024, 128), 0) * 4 + row).astype(F32)

        def body(k, carry):
            for half in range(2):
                hit = slots == pos[k * 2 + half, 0:1, :]
                pm[k, :, half * 128 : half * 128 + 128] = jnp.where(hit, 1.0, 0.0).astype(BF16)
            return carry

        lax.fori_loop(k0, k1, body, 0)

    barrier = pltpu.get_barrier_semaphore()
    peers = [cube_dev(fl) for fl in CUBE] + [far_dev(fl) for fl in FAR] + [partner]
    for dev in peers:
        pl.semaphore_signal(barrier, inc=1, device_id=dev, device_id_type=MESH)
    inputs = [
        pltpu.make_async_copy(src, dst, inp.at[k])
        for k, (src, dst) in enumerate(
            ((ids_in, ids_ref), (rows_in, rows_ref), (embed_in, embed_ref), (gain_in, gain_ref))
        )
    ]
    for copy in inputs:
        copy.start()
    load_own(0)
    for k in range(2):
        idf[g_me, k, b_me] = jnp.zeros((8, 128), jnp.int32)
    pl.semaphore_wait(barrier, len(peers))
    w1_send(0)
    for l in range(1, LAYERS):
        load_own(l)

    inputs[0].wait()
    ids = 8.0 - ids_ref[...].astype(F32)
    i0 = lax.broadcasted_iota(jnp.int32, (32, 32), 0)
    i1 = lax.broadcasted_iota(jnp.int32, (32, 32), 1)
    code = jnp.sum(jnp.where(i0 == i1, ids, 0.0), axis=1, keepdims=True)
    lane = lax.broadcasted_iota(jnp.int32, (32, 128), 1)
    sub = lax.broadcasted_iota(jnp.int32, (32, 128), 0)
    line = jnp.sum(jnp.where(lane == sub + (col % 4) * 32, code, 0.0), axis=0, keepdims=True)
    idg[zo, yo * 2 + x, 0:1] = line.astype(jnp.int32)
    for copy in inputs[1:]:
        copy.wait()
    own_rows = pl.ds(pl.multiple_of(yo * 64 + x * 32, 32), 32)
    square = jnp.zeros((32, 128), F32)
    for q in range(8):
        for k in range(4):
            zz = q // 4 if k < 2 else 3 - q // 4
            yy = (q // 2) % 2 if k % 2 == 0 else 3 - (q // 2) % 2
            c = (zz * 8 + yy * 2 + q % 2) * 128
            lanes = slice(k * 128, k * 128 + 128)
            table = embed_ref[:, c : c + 128].astype(F32)
            term = jnp.zeros((32, 128), F32)
            for t in range(8):
                term = jnp.where(code == 8.0 - t, table[t : t + 1], term)
            start = (rows_ref[:, c : c + 128].astype(F32) + term).astype(BF16)
            a[0, q, zo, own_rows, lanes] = start
            start = start.astype(F32)
            square = square + start * start
            for l in range(LAYERS):
                gp[l, q, 0:1, lanes] = gain_ref[l : l + 1, c : c + 128]
    for k in range(7):
        id1(k).start()
    step1(0, 0)
    step1(0, 1)
    total = jnp.sum(square, axis=1, keepdims=True)
    line = jnp.sum(jnp.where(lane == sub + yo * 64 + x * 32, total, 0.0), axis=0, keepdims=True)
    stat[0, zo, qme, 0:1] = line
    stat[0, 1 - zo, qme, 0:1] = jnp.zeros((1, 128), F32)
    for k in range(7):
        stat_copy(0, k, 0).start()
        stat_copy(0, k, 1).start()

    step2(0, 0)
    arrived(seven, i1r)
    for k in range(2):
        idf[g_me, k, b_me, 0:1] = idg[k, 0, 0:1] + idg[k, 1, 0:1] + idg[k, 2, 0:1] + idg[k, 3, 0:1]
    for k in range(7):
        id2(k).start()
    w1_first(0)
    w1_send(1)
    step2(0, 1)
    step3(0, 0)
    read_stats(0, 0)
    read_stats(0, 1)
    step3(0, 1)
    w1_rest(0)

    def activate_both(q, carry):
        activate(0, 0, q)
        activate(0, 1, q)
        return carry

    step3_in(0, 0)
    lax.fori_loop(0, 4, activate_both, 0)
    arrived(idf.at[pl.ds(0, 7), :, 0], i2r)
    for k in range(2):
        id3(k).start()
    step3_in(0, 1)
    lax.fori_loop(4, 8, activate_both, 0)
    mine = [core * 4 + k for k in range(4)]
    others = [(1 - core) * 4 + k for k in range(4)]
    w2_in(0)
    for i in range(2):
        multiply(0, i, mine, True)
    wd_in(0)
    for i in range(2):
        multiply(0, i, others, False)
        finish(0, i, a[0, qme, i])
        begin(1, i)

    arrived(idf.at[pl.ds(0, 4)], i3r)
    positions()
    selection(0, 8)

    def layer(l, carry):
        near = [cube_q(CUBE[d]) for d in range(3)]
        mid = [cube_q(pair(d)) for d in range(3)]
        w1_first(l)

        @pl.when(l < LAYERS - 1)
        def _():
            w1_send(l + 1)

        read_stats(l, 0)
        activate(l, 0, qme)
        step2(l, 0)
        read_stats(l, 1)
        activate(l, 1, qme)
        step2(l, 1)
        for q in near:
            activate(l, 0, q)
        step3(l, 0)
        for q in near:
            activate(l, 1, q)
        w1_rest(l)
        step3(l, 1)

        for q in mid:
            activate(l, 0, q)
        for q in mid:
            activate(l, 1, q)

        most = [qme] + near + mid

        @pl.when(l == 1)
        def _():
            selection(8, 16)
            drain_act(0)
            left(seven, i1s)
            left(idf.at[pl.ds(0, 7), :, 0], i2s)
            left(idf.at[pl.ds(0, 4)], i3s)

        @pl.when(l >= 2)
        def _():
            drain_act(l - 1)

        w2_in(l)
        drain_stats(l - 1)
        drain_weights(l - 1)
        wd_in(l)
        for i in range(2):
            multiply(l, i, most, True)
            step3_in(l, i)
            activate(l, i, cube_q(ALL))
            multiply(l, i, [cube_q(ALL)], False)
            finish(l, i, a[l, qme, i])

            @pl.when(l < LAYERS - 1)
            def _():
                begin(l + 1, i)

            @pl.when(l == LAYERS - 1)
            def _():
                out_begin(i)

        return carry

    lax.fori_loop(1, LAYERS, layer, 0)

    out2(0).start()
    drain_weights(LAYERS - 1)
    drain_act(LAYERS - 1)
    drain_stats(LAYERS - 1)

    def place(first, last, groups):
        for m in range(4):
            lines = slice(m * 256, m * 256 + 256)
            total = None
            for at in groups:
                for k in range(2):
                    part = jnp.dot(
                        pm[at * 2 + k, lines], f[at, k].reshape(256, 128), preferred_element_type=F32
                    )
                    total = part if total is None else total + part
            if not first:
                total = total + oacc[lines]
            if last:
                out_ref[lines] = total.astype(BF16)
            else:
                oacc[lines] = total

    for k in range(3):
        arrived(f.at[0, :, 0], fr.at[k])
        out2(k + 1).start()
    place(True, False, [(xh * 2 + core) * 2 + k for k in range(2)])
    arrived(f.at[pl.ds(0, 2)], fdr.at[0])
    place(False, False, [(xh * 2 + 1 - core) * 2 + k for k in range(2)])
    for k in range(3, 7):
        arrived(f.at[0, :, 0], fr.at[k])
        out2(k + 1).start()
    place(False, False, [((1 - xh) * 2 + core) * 2 + k for k in range(2)])
    arrived(f.at[0], fdr.at[1])
    place(False, False, [((1 - xh) * 2 + 1 - core) * 2 + zh])
    arrived(f.at[0], fdr.at[2])
    place(False, True, [((1 - xh) * 2 + 1 - core) * 2 + 1 - zh])

    left(f.at[pl.ds(0, 7), :, 0], fs)
    left(f.at[pl.ds(0, 4)], fds)


def shards(rows, task_ids, task_embed, norm_gain, layer_weight):
    dma = pltpu.SemaphoreType.DMA
    vmem = pltpu.VMEM
    return pl.pallas_call(
        kernel,
        out_shape=pltpu.VMEM((1024, 128), BF16),
        in_specs=[pl.BlockSpec(memory_space=pl.ANY)] * 5,
        out_specs=pl.BlockSpec(memory_space=pltpu.VMEM),
        scratch_shapes=[
            vmem((32, 4096), BF16),
            vmem((1, 32), jnp.int32),
            vmem((8, 4096), BF16),
            vmem((4, 4096), F32),
            vmem((4, 4, 8, 4, 128, 128), BF16),
            vmem((5, 8, 2, 128, 512), BF16),
            vmem((8, 2, 128, 512), BF16),
            vmem((2, 128, 512), F32),
            vmem((4, 8, 8, 512), F32),
            vmem((16, 1024, 256), BF16),
            vmem((8, 2, 2, 128, 128), BF16),
            vmem((2, 4, 8, 128), jnp.int32),
            vmem((8, 2, 2, 8, 128), jnp.int32),
            vmem((32, 8, 128), F32),
            vmem((5, 2, 8, 8, 128), F32),
            vmem((2, 128, 128), F32),
            vmem((1024, 128), F32),
            dma((4,)),
            dma((4,)),
            dma((4,)),
            dma((4, 2)),
            dma((4,)),
            dma((4,)),
            dma((4,)),
            dma((4, 2)),
            dma((4, 2)),
            dma((4, 2)),
            dma((4,)),
            dma((4, 2)),
            *[dma] * 6,
            dma,
            dma((7,)),
            dma,
            dma((3,)),
        ],
        compiler_params=pltpu.CompilerParams(
            collective_id=0, has_side_effects=True, vmem_limit_bytes=60 * 1024 * 1024
        ),
    )(
        rows,
        task_ids.reshape(1, 32),
        task_embed,
        norm_gain,
        layer_weight.reshape(4, 4, 4, 2, 128, 128),
    )


def solution(mesh):
    return jax.shard_map(
        shards,
        mesh=mesh,
        in_specs=(P(("row", "col"), None), P(("row", "col")), P(), P(), P(None, None, "col")),
        out_specs=P("row", "col"),
        check_vma=False,
    )
```
